32 devices in a mesh: data: 4 (over y, z), ctx: 8 (over x, core).
Axes of the slice: x: 4, y: 2, z: 2, core: 2. Of those that a mesh axis runs over, the one named last changes fastest.
The devices are a block of a 4x4x8 slice.
Arguments:
- hidden: bfloat16 [1024, 5120], P(('data', 'ctx')), parts along dimension 0
- seq_lens: int32 [1024], P(('data', 'ctx')), parts along dimension 0
- w_query: bfloat16 [2, 5120, 4096], replicated
- w_key: bfloat16 [2, 5120, 1024], replicated
- w_value: bfloat16 [2, 5120, 1024], replicated
- w_out: bfloat16 [2, 4096, 5120], replicated
- k_prefix: bfloat16 [2, 8192, 8, 128], P(None, ('data', 'ctx')), parts along dimension 1
- v_prefix: bfloat16 [2, 8192, 8, 128], P(None, ('data', 'ctx')), parts along dimension 1
- k_suffix: bfloat16 [2, 1024, 32, 8, 128], P(None, ('data', 'ctx')), parts along dimension 1
- v_suffix: bfloat16 [2, 1024, 32, 8, 128], P(None, ('data', 'ctx')), parts along dimension 1
Outputs:
- output 1: bfloat16 [1024, 5120], P(('data', 'ctx')), parts along dimension 0
- output 2: bfloat16 [2, 1024, 32, 8, 128], P(None, ('data', 'ctx')), parts along dimension 1
- output 3: bfloat16 [2, 1024, 32, 8, 128], P(None, ('data', 'ctx')), parts along dimension 1
There are 4 independent parts. The reference program is written for one: setup_inputs(seed, part) draws one part's arguments, and reference() takes and returns one part's arrays. A program takes and returns all parts, laid end to end along the dimension named above; an argument that names none is the same for every part.
All inputs are finite; a program needn't handle non-finite values.
Results may differ from the reference program's by a relative error of at most 0.0105281.
Values are sent between devices in bfloat16 or wider.
A program may use at most 768 MiB of HBM per device.

```python
import jax
import jax.numpy as jnp
from jax import lax

MODEL_DIM = 5120
NUM_HEADS = 32
KV_HEADS = 8
HEAD_DIM = 128
LAYERS = 2
SHARDS = 8
BATCH_SIZE = 256
PREFIX_LEN = 2048
SUFFIX_LEN = 32
HOME_ROWS = 32


def setup_inputs(seed: int = 0, part: int = 0) -> dict:
    shared_keys = jax.random.split(jax.random.key(seed), 4)
    part_keys = jax.random.split(jax.random.fold_in(jax.random.key(seed + 1), part), 10)
    q_width = NUM_HEADS * HEAD_DIM
    kv_width = KV_HEADS * HEAD_DIM
    shard_rows = PREFIX_LEN // SHARDS
    w_query = jax.random.normal(shared_keys[0], (LAYERS, MODEL_DIM, q_width), jnp.float32) * MODEL_DIM ** -0.5
    w_key = jax.random.normal(shared_keys[1], (LAYERS, MODEL_DIM, kv_width), jnp.float32) * (2.5 * MODEL_DIM ** -0.5)
    w_value = jax.random.normal(shared_keys[2], (LAYERS, MODEL_DIM, kv_width), jnp.float32) * MODEL_DIM ** -0.5
    w_out = jax.random.normal(shared_keys[3], (LAYERS, q_width, MODEL_DIM), jnp.float32) * (q_width * LAYERS) ** -0.5
    hidden = jax.random.normal(part_keys[0], (BATCH_SIZE, MODEL_DIM), jnp.float32)
    centre_shape = (LAYERS, SHARDS, 1, KV_HEADS, HEAD_DIM)
    block_shape = (LAYERS, SHARDS, shard_rows, KV_HEADS, HEAD_DIM)
    prefix_shape = (LAYERS, PREFIX_LEN, KV_HEADS, HEAD_DIM)
    k_prefix = (1.5 * jax.random.normal(part_keys[1], centre_shape, jnp.float32) + jax.random.normal(part_keys[2], block_shape, jnp.float32)).reshape(prefix_shape)
    v_prefix = (jax.random.normal(part_keys[3], centre_shape, jnp.float32) + 0.5 * jax.random.normal(part_keys[4], block_shape, jnp.float32)).reshape(prefix_shape)
    seq_centre = (LAYERS, BATCH_SIZE, 1, KV_HEADS, HEAD_DIM)
    suffix_shape = (LAYERS, BATCH_SIZE, SUFFIX_LEN, KV_HEADS, HEAD_DIM)
    k_suffix = 2.5 * jax.random.normal(part_keys[5], seq_centre, jnp.float32) + jax.random.normal(part_keys[6], suffix_shape, jnp.float32)
    v_suffix = jax.random.normal(part_keys[7], seq_centre, jnp.float32) + 0.5 * jax.random.normal(part_keys[8], suffix_shape, jnp.float32)
    len_keys = jax.random.split(part_keys[9], 2)
    seq_lens = jax.random.randint(len_keys[0], (BATCH_SIZE,), 0, SUFFIX_LEN, dtype=jnp.int32)
    longest = jax.random.randint(len_keys[1], (), 0, BATCH_SIZE, dtype=jnp.int32)
    seq_lens = seq_lens.at[longest].set(SUFFIX_LEN - 1)
    seq_lens = seq_lens.at[(longest + BATCH_SIZE // 2) % BATCH_SIZE].set(0)
    return {'hidden': hidden.astype(jnp.bfloat16), 'seq_lens': seq_lens, 'w_query': w_query.astype(jnp.bfloat16), 'w_key': w_key.astype(jnp.bfloat16), 'w_value': w_value.astype(jnp.bfloat16), 'w_out': w_out.astype(jnp.bfloat16), 'k_prefix': k_prefix.astype(jnp.bfloat16), 'v_prefix': v_prefix.astype(jnp.bfloat16), 'k_suffix': k_suffix.astype(jnp.bfloat16), 'v_suffix': v_suffix.astype(jnp.bfloat16)}


def attend_block(queries, k_pre, v_pre, k_suf, v_suf, slot_live):
    score_scale = HEAD_DIM ** -0.5
    pre_scores = jnp.einsum('bkgd,pkd->bkgp', queries, k_pre) * score_scale
    suf_scores = jnp.einsum('bkgd,bskd->bkgs', queries, k_suf) * score_scale
    suf_scores = jnp.where(slot_live[:, None, None, :], suf_scores, -jnp.inf)
    row_max = jnp.maximum(pre_scores.max(axis=-1), suf_scores.max(axis=-1))
    pre_exp = jnp.exp(pre_scores - row_max[..., None])
    suf_exp = jnp.exp(suf_scores - row_max[..., None])
    mass_sum = pre_exp.sum(axis=-1) + suf_exp.sum(axis=-1)
    mixed_sum = jnp.einsum('bkgp,pkd->bkgd', pre_exp, v_pre) + jnp.einsum('bkgs,bskd->bkgd', suf_exp, v_suf)
    return mixed_sum / mass_sum[..., None]


def reference(hidden, seq_lens, w_query, w_key, w_value, w_out, k_prefix, v_prefix, k_suffix, v_suffix):
    group_size = NUM_HEADS // KV_HEADS
    blocks = BATCH_SIZE // HOME_ROWS
    slot_ids = jnp.arange(SUFFIX_LEN, dtype=jnp.int32)[None, :]
    slot_hit = (slot_ids == seq_lens[:, None])[:, :, None, None]
    slot_live = slot_ids <= seq_lens[:, None]
    live_blocks = slot_live.reshape(blocks, HOME_ROWS, SUFFIX_LEN)

    def layer_step(hidden_state, layer_args):
        q_weight, k_weight, v_weight, o_weight, k_pre, v_pre, k_suf, v_suf = layer_args
        queries = jnp.dot(hidden_state, q_weight, preferred_element_type=jnp.float32).astype(jnp.bfloat16)
        k_new = jnp.dot(hidden_state, k_weight, preferred_element_type=jnp.float32).astype(jnp.bfloat16).reshape(BATCH_SIZE, 1, KV_HEADS, HEAD_DIM)
        v_new = jnp.dot(hidden_state, v_weight, preferred_element_type=jnp.float32).astype(jnp.bfloat16).reshape(BATCH_SIZE, 1, KV_HEADS, HEAD_DIM)
        k_suf = jnp.where(slot_hit, k_new, k_suf)
        v_suf = jnp.where(slot_hit, v_new, v_suf)
        q_blocks = queries.astype(jnp.float32).reshape(blocks, HOME_ROWS, KV_HEADS, group_size, HEAD_DIM)
        k_full = k_pre.astype(jnp.float32)
        v_full = v_pre.astype(jnp.float32)
        k_blocks = k_suf.astype(jnp.float32).reshape(blocks, HOME_ROWS, SUFFIX_LEN, KV_HEADS, HEAD_DIM)
        v_blocks = v_suf.astype(jnp.float32).reshape(blocks, HOME_ROWS, SUFFIX_LEN, KV_HEADS, HEAD_DIM)
        attended = lax.map(lambda block_args: attend_block(block_args[0], k_full, v_full, block_args[1], block_args[2], block_args[3]), (q_blocks, k_blocks, v_blocks, live_blocks))
        attended = attended.astype(jnp.bfloat16).reshape(BATCH_SIZE, NUM_HEADS * HEAD_DIM)
        update = jnp.dot(attended, o_weight, preferred_element_type=jnp.float32).astype(jnp.bfloat16)
        hidden_state = (hidden_state.astype(jnp.float32) + update.astype(jnp.float32)).astype(jnp.bfloat16)
        return hidden_state, (k_suf, v_suf)

    hidden_out, cache_out = lax.scan(layer_step, hidden, (w_query, w_key, w_value, w_out, k_prefix, v_prefix, k_suffix, v_suffix))
    return hidden_out, cache_out[0], cache_out[1]
```

```python
import functools

import jax
import jax.numpy as jnp
from jax import lax
from jax.experimental import pallas as pl
from jax.experimental.pallas import tpu as pltpu
from jax.sharding import PartitionSpec as P

MESH = pl.DeviceIdType.MESH
BF16 = jnp.bfloat16
F32 = jnp.float32
RING = 10
COLS = 512
LOG2E = 1.4426950408889634
FLOOR = float(jnp.finfo(jnp.float32).min)


def dot(a, b):
    return lax.dot_general(a, b, (((1,), (0,)), ((), ())), preferred_element_type=F32)


def dot_t(a, b):
    return lax.dot_general(a, b, (((1,), (1,)), ((), ())), preferred_element_type=F32)


def decode_kernel(ctx_size, hidden, lens, wq, wk, wv, wo, kpre, vpre, ksuf, vsuf, hid_out, kvn_out,
                  wq_ring, wkv_ring, w_sem, wo_buf, wo_sem, pst, pst_sem, pf32, psend, precv, ps_s, ps_r,
                  suf, suf_sem, xr, xr_sem, xh, fin_st, fin_rc, x_sem, acc_q, acc_kv, qkv_st, hq, hs_s, hs_r,
                  q_rc, q_s, q_r, qs, os, ls, sc, pb, o_st, lse_st, o_rc, lse_rc, o_s, o_r, l_s, l_r,
                  o_cat, oc_s, oc_r, acc_o):
    layers = wq.shape[0]
    dim = wq.shape[1]
    half = dim // 2
    kc = dim // 4
    rows, heads, hd = hidden.shape[0], kpre.shape[2], kpre.shape[3]
    group = wq.shape[2] // (heads * hd)
    span = kpre.shape[1]
    slots = ksuf.shape[2] // heads
    chips = ctx_size // 2
    order = (2, 1, 3, 0)
    scale = hd ** -0.5
    c2 = scale * LOG2E
    gq = group * hd
    nblk = half // COLS

    me = lax.axis_index("ctx")
    chip = me // 2
    core = me % 2
    other = 1 - core
    partner = chip * 2 + other
    pending = []

    def to(dev):
        return {"ctx": dev}

    def remote(src, dst, s_sem, r_sem, dev):
        return pltpu.make_async_remote_copy(src_ref=src, dst_ref=dst, send_sem=s_sem, recv_sem=r_sem,
                                            device_id=to(dev), device_id_type=MESH)

    def send(src, dst, s_sem, r_sem, dev):
        copy = remote(src, dst, s_sem, r_sem, dev)
        copy.start()
        pending.append(copy)

    def arrived(dst, r_sem, s_sem):
        remote(dst, dst, s_sem, r_sem, partner).wait_recv()

    def dest_chip(t):
        return (chip + order[t]) % chips

    def src_chip(t):
        return (chip + chips - order[t]) % chips

    def weight_copies(layer, t, hh, kk):
        slot = (layer * 16 + t * 4 + hh * 2 + kk) % RING
        g = dest_chip(t) * 2 + core
        row = pl.multiple_of(((core + hh) % 2) * half + kk * kc, 128)
        krows = pl.ds(row, kc)
        return (
            pltpu.make_async_copy(wq.at[layer, krows, pl.ds(pl.multiple_of(g * gq, gq), gq)],
                                  wq_ring.at[slot], w_sem.at[slot, 0]),
            pltpu.make_async_copy(wk.at[layer, krows, pl.ds(pl.multiple_of(g * hd, hd), hd)],
                                  wkv_ring.at[slot, :, 0:hd], w_sem.at[slot, 1]),
            pltpu.make_async_copy(wv.at[layer, krows, pl.ds(pl.multiple_of(g * hd, hd), hd)],
                                  wkv_ring.at[slot, :, hd:2 * hd], w_sem.at[slot, 2]),
        )

    def fetch_weights(layer, first, last):
        for n in range(first, min(last, 4 * chips)):
            for copy in weight_copies(layer, n // 4, (n // 2) % 2, n % 2):
                copy.start()

    def wo_copy(layer, tc, nb):
        return pltpu.make_async_copy(
            wo.at[layer, pl.ds(pl.multiple_of(tc * 2 * gq, 2 * gq), 2 * gq),
                  pl.ds(pl.multiple_of(core * half + nb * COLS, COLS), COLS)],
            wo_buf.at[tc, nb], wo_sem.at[tc, nb])

    def fetch_wo(layer, tc):
        for nb in range(nblk):
            wo_copy(layer, tc, nb).start()

    def prefix_copies(layer):
        return (pltpu.make_async_copy(kpre.at[layer], pst.at[0], pst_sem.at[0]),
                pltpu.make_async_copy(vpre.at[layer], pst.at[1], pst_sem.at[1]))

    def suffix_copies(layer):
        return (pltpu.make_async_copy(ksuf.at[layer], suf.at[0], suf_sem.at[0]),
                pltpu.make_async_copy(vsuf.at[layer], suf.at[1], suf_sem.at[1]))

    def relayout_prefix(layer):
        for copy in prefix_copies(layer):
            copy.wait()
        step = 64

        @pl.loop(0, 2)
        def _(kv):
            @pl.loop(0, span // step)
            def _(blk):
                base = pl.multiple_of(blk * step, step)
                pf32[...] = pst[kv, pl.ds(base, step)].astype(F32).reshape(step * heads, hd)
                for g in range(heads):
                    psend[layer, g, kv, pl.ds(base, step), :] = pf32[pl.ds(g, step, stride=heads), :].astype(BF16)

    def send_prefix(layer):
        for d in (4, 5, 3, 2, 6, 7, 1):
            dev = (me + d) % ctx_size
            send(psend.at[layer, dev], precv.at[layer, :, me], ps_s.at[layer, dev], ps_r.at[layer, me], dev)
        for kv in range(2):
            precv[layer, kv, me] = psend[layer, me, kv]

    def await_prefix(layer):
        for d in (1, 7, 2, 6, 3, 5, 4):
            src = (me + d) % ctx_size
            arrived(precv.at[layer, :, src], ps_r.at[layer, src], ps_s.at[layer, src])

    def project(layer, t):
        acc_q[...] = jnp.zeros_like(acc_q)
        acc_kv[...] = jnp.zeros_like(acc_kv)

        for n in range(4 * t, 4 * t + 4):
            hh, kk = (n // 2) % 2, n % 2
            slot = (layer * 16 + n) % RING
            for copy in weight_copies(layer, t, hh, kk):
                copy.wait()
            lhs = xh[layer, (core + hh) % 2, :, kk * kc:(kk + 1) * kc]
            acc_q[...] += dot(lhs, wq_ring[slot])
            acc_kv[...] += dot(lhs, wkv_ring[slot])
            fetch_weights(layer, n + RING, n + RING + 1)
            if layer == 0 and t == 2:
                fetch_wo(0, n % 4)

        q = acc_q[...].astype(BF16)
        kv = acc_kv[...].astype(BF16)
        for cr in range(2):
            part = slice(cr * rows, (cr + 1) * rows)
            for j in range(group):
                qkv_st[layer, t, cr, j] = q[part, j * hd:(j + 1) * hd]
            qkv_st[layer, t, cr, group] = kv[part, 0:hd]
            qkv_st[layer, t, cr, group + 1] = kv[part, hd:2 * hd]
        tc = dest_chip(t)
        if order[t] != 0:
            send(qkv_st.at[layer, t, :, 0:group], q_rc.at[layer, chip], q_s.at[layer, t], q_r.at[layer, chip],
                 tc * 2 + core)
        else:
            q_rc[layer, chip] = qkv_st[layer, t, :, 0:group]
        g = tc * 2 + core
        send(qkv_st.at[layer, t, other], hq.at[layer, g], hs_s.at[layer, t], hs_r.at[layer, t], partner)
        hq[layer, g] = qkv_st[layer, t, core]

    def suffix_attention(layer):
        for t in range(chips):
            arrived(hq.at[layer, dest_chip(t) * 2 + other], hs_r.at[layer, t], hs_s.at[layer, t])
        for g in range(heads):
            for j in range(group):
                qs[pl.ds(g * group + j, rows, stride=heads * group), :] = hq[layer, g, j].astype(F32)
        for copy in suffix_copies(layer):
            copy.wait()
        qh = heads * group
        row_id = lax.broadcasted_iota(jnp.int32, (qh, slots * heads), 0)
        col_id = lax.broadcasted_iota(jnp.int32, (qh, slots * heads), 1)
        slot_of = jnp.where((row_id // group) == (col_id % heads), col_id // heads, slots)
        step = 8

        @pl.loop(0, rows // step)
        def _(blk):
            for i in range(step):
                b = blk * step + i
                base = pl.multiple_of(b * qh, qh)
                s = dot_t(qs[pl.ds(base, qh), :].astype(BF16), suf[0, b])
                s = jnp.where(slot_of < lens[b], s, FLOOR)
                m = jnp.max(s, axis=1, keepdims=True)
                e = jnp.exp2((s - m) * c2)
                mass = jnp.sum(e, axis=1, keepdims=True)
                val = dot(e.astype(BF16), suf[1, b])
                os[pl.ds(base, qh), :] = val * (1.0 / mass)
                ls[pl.ds(base, qh), :] = jnp.broadcast_to(m * scale + jnp.log(mass), (qh, hd))

    def prefix_attention(layer, t):
        src = src_chip(t)
        if order[t] != 0:
            arrived(q_rc.at[layer, src], q_r.at[layer, src], q_s.at[layer, t])
        q = q_rc[layer, src].reshape(2 * group * rows, hd)
        peak = None
        for s in range(ctx_size):
            part = dot_t(q, precv[layer, 0, s])
            sc[s] = part
            for lo in range(0, span, 128):
                piece = part[:, lo:lo + 128]
                peak = piece if peak is None else jnp.maximum(peak, piece)
        m = jnp.max(peak, axis=1, keepdims=True)
        mass = jnp.zeros((2 * group * rows, 128), F32)
        for s in range(ctx_size):
            e = jnp.exp2((sc[s] - m) * c2)
            for lo in range(0, span, 128):
                mass = mass + e[:, lo:lo + 128]
            pb[:, s * span:(s + 1) * span] = e.astype(BF16)
        mass = jnp.sum(mass, axis=1, keepdims=True)
        vals = dot(pb[...], precv[layer, 1].reshape(ctx_size * span, hd))
        out = (vals * (1.0 / mass)).astype(BF16)
        lse = jnp.broadcast_to(m * scale + jnp.log(mass), (2 * group * rows, 128)).T
        for cr in range(2):
            part = group * rows
            o_st[layer, t, cr] = out[cr * part:(cr + 1) * part].reshape(group, rows, hd)
            lse_st[layer, t, cr] = lse[0:8, cr * part:(cr + 1) * part]
        if order[t] != 0:
            for cr in range(2):
                dev = src * 2 + cr
                send(lse_st.at[layer, t, cr], lse_rc.at[layer, me], l_s.at[layer, t, cr], l_r.at[layer, me], dev)
                send(o_st.at[layer, t, cr], o_rc.at[layer, me], o_s.at[layer, t, cr], o_r.at[layer, me], dev)
        else:
            send(lse_st.at[layer, t, other], lse_rc.at[layer, me], l_s.at[layer, t, 0], l_r.at[layer, me], partner)
            send(o_st.at[layer, t, other], o_rc.at[layer, me], o_s.at[layer, t, 0], o_r.at[layer, me], partner)
            lse_rc[layer, me] = lse_st[layer, t, core]
            o_rc[layer, me] = o_st[layer, t, core]

    def combine(layer, t):
        tc = dest_chip(t)
        for par in range(2):
            if order[t] != 0:
                g = tc * 2 + par
                arrived(lse_rc.at[layer, g], l_r.at[layer, g], l_s.at[layer, t, 0])
                arrived(o_rc.at[layer, g], o_r.at[layer, g], o_s.at[layer, t, 0])
            elif par == 0:
                arrived(lse_rc.at[layer, partner], l_r.at[layer, partner], l_s.at[layer, t, 0])
                arrived(o_rc.at[layer, partner], o_r.at[layer, partner], o_s.at[layer, t, 0])
        for par in range(2):
            g = tc * 2 + par
            lse_p = jnp.broadcast_to(lse_rc[layer, g, 0:1, :], (group * rows, 128)).T
            k_new = hq[layer, g, group].astype(F32)
            v_new = hq[layer, g, group + 1].astype(F32)
            for j in range(group):
                h = g * group + j
                picked = pl.ds(h, rows, stride=heads * group)
                lp = lse_p[j * rows:(j + 1) * rows]
                lo = ls[picked, :]
                sn = jnp.sum(hq[layer, g, j].astype(F32) * k_new, axis=1, keepdims=True) * scale
                top = jnp.maximum(jnp.maximum(lp, lo), sn)
                wp = jnp.exp(lp - top)
                wo_ = jnp.exp(lo - top)
                wn = jnp.exp(sn - top)
                mixed = wp * o_rc[layer, g, j].astype(F32) + wo_ * os[picked, :] + wn * v_new
                at = (par * group + j) * hd
                o_cat[layer, core, tc, :, at:at + hd] = (mixed / (wp + wo_ + wn)).astype(BF16)
        send(o_cat.at[layer, core, tc], o_cat.at[layer, core, tc], oc_s.at[layer, t], oc_r.at[layer, t], partner)

    def project_out(layer, t):
        tc = dest_chip(t)
        arrived(o_cat.at[layer, other, tc], oc_r.at[layer, t], oc_s.at[layer, t])
        lhs = jnp.concatenate([o_cat[layer, 0, tc], o_cat[layer, 1, tc]], axis=0)

        @pl.loop(0, nblk)
        def _(nb):
            wo_copy(layer, tc, nb).wait()
            upd = dot(lhs, wo_buf[tc, nb])
            if t == 0:
                acc_o[nb] = upd
            else:
                acc_o[nb] += upd
            if layer + 1 < layers:
                wo_copy(layer + 1, tc, nb).start()

    for copy in prefix_copies(0):
        copy.start()
    fetch_weights(0, 0, 4)
    barrier = pltpu.get_barrier_semaphore()
    for d in range(1, ctx_size):
        pl.semaphore_signal(barrier, inc=1, device_id=to((me + d) % ctx_size), device_id_type=MESH)
    pl.semaphore_wait(barrier, ctx_size - 1)
    send(hidden, xr.at[core], xr_sem.at[0], xr_sem.at[1], partner)
    fetch_weights(0, 4, RING)
    xr[core] = hidden[...]
    relayout_prefix(0)
    send_prefix(0)
    arrived(xr.at[other], xr_sem.at[1], xr_sem.at[0])
    for sd in range(2):
        for cr in range(2):
            xh[0, sd, cr * rows:(cr + 1) * rows, :] = xr[cr, :, sd * half:(sd + 1) * half]

    for layer in range(layers):
        for t in range(chips):
            project(layer, t)
            if layer == 0 and t == 1:
                for copy in suffix_copies(0):
                    copy.start()
        if layer + 1 < layers:
            for copy in prefix_copies(layer + 1):
                copy.start()
            fetch_weights(layer + 1, 0, RING)
            suffix_attention(layer)
            for copy in suffix_copies(layer + 1):
                copy.start()
            relayout_prefix(layer + 1)
        await_prefix(layer)
        for t in range(chips):
            prefix_attention(layer, t)
        if layer + 1 < layers:
            send_prefix(layer + 1)
        else:
            suffix_attention(layer)
        for t in range(chips):
            combine(layer, t)
            if t > 0:
                project_out(layer, t - 1)
        project_out(layer, chips - 1)
        for nb in range(nblk):
            cols = slice(nb * COLS, (nb + 1) * COLS)
            new = (xh[layer, core, :, cols].astype(F32) + acc_o[nb].astype(BF16).astype(F32)).astype(BF16)
            if layer + 1 < layers:
                xh[layer + 1, core, :, cols] = new
            else:
                for cr in range(2):
                    fin_st[cr, :, cols] = new[cr * rows:(cr + 1) * rows]
        if layer + 1 < layers:
            send(xh.at[layer + 1, core], xh.at[layer + 1, core], x_sem.at[0, 0], x_sem.at[0, 1], partner)
            arrived(xh.at[layer + 1, other], x_sem.at[0, 1], x_sem.at[0, 0])
    send(fin_st.at[other], fin_rc, x_sem.at[1, 0], x_sem.at[1, 1], partner)
    hid_out[core] = fin_st[core]
    for layer in range(layers):
        for g in range(heads):
            for i in range(2):
                kvn_out[layer, g, i] = hq[layer, g, group + i]
    arrived(fin_rc, x_sem.at[1, 1], x_sem.at[1, 0])
    hid_out[other] = fin_rc[...]
    for copy in pending:
        copy.wait_send()


def cache_kernel(lens, hid, kvn, ksuf, vsuf, hid_out, kout, vout, buf, tiles, in_sem, out_sem):
    layers, batch = ksuf.shape[0], ksuf.shape[1]
    heads, hd = ksuf.shape[3], ksuf.shape[4]
    half = hid.shape[2]
    step = 8
    parts = batch // step
    srcs, dsts = (ksuf, vsuf), (kout, vout)

    def copies(layer, i, part, out):
        here = pl.ds(part * step, step)
        at = (layer * 2 + i) * parts + part
        if out:
            return pltpu.make_async_copy(buf.at[layer, i, here], dsts[i].at[layer, here], out_sem.at[at])
        return pltpu.make_async_copy(srcs[i].at[layer, here], buf.at[layer, i, here], in_sem.at[at])

    todo = [(layer, i, part) for layer in range(layers) for i in range(2) for part in range(parts)]
    for layer, i, part in todo:
        copies(layer, i, part, False).start()
    for sd in range(2):
        hid_out[:, sd * half:(sd + 1) * half] = hid[sd]
    for layer in range(layers):
        for i in range(2):
            for g in range(heads):
                tiles[layer, i, pl.ds(g, batch, stride=heads), :] = kvn[layer, g, i].astype(F32)
    for layer, i, part in todo:
        copies(layer, i, part, False).wait()
        for b in range(part * step, (part + 1) * step):
            buf[layer, i, b, lens[b]] = tiles[layer, i, b * heads:(b + 1) * heads, :].astype(BF16)
        copies(layer, i, part, True).start()
    for layer, i, part in todo:
        copies(layer, i, part, True).wait()


def solution(mesh):
    ctx_size = mesh.shape["ctx"]
    home = ("data", "ctx")
    row_spec, lens_spec, whole = P(home, None), P(home), P()
    prefix_spec = P(None, home, None, None)
    cache_spec = P(None, home, None, None, None)

    def local_step(hidden, seq_lens, w_query, w_key, w_value, w_out, k_prefix, v_prefix, k_suffix, v_suffix):
        layers, dim, q_width = w_query.shape
        rows = hidden.shape[0]
        span, heads, hd = k_prefix.shape[1:]
        slots = k_suffix.shape[2]
        group = q_width // (heads * hd)
        chips = ctx_size // 2
        half, kc = dim // 2, dim // 4
        nblk = half // COLS
        qh = heads * group
        vmem, smem, anym = pltpu.VMEM, pltpu.SMEM, pl.ANY
        dma = pltpu.SemaphoreType.DMA
        spec = pl.BlockSpec
        scratch = [
            vmem((RING, kc, group * hd), BF16), vmem((RING, kc, 2 * hd), BF16), dma((RING, 3)),
            vmem((chips, nblk, 2 * group * hd, COLS), BF16), dma((chips, nblk)),
            vmem((2, span, heads, hd), BF16), dma((2,)), vmem((64 * heads, hd), F32),
            vmem((layers, ctx_size, 2, span, hd), BF16), vmem((layers, 2, ctx_size, span, hd), BF16),
            dma((layers, ctx_size)), dma((layers, ctx_size)),
            vmem((2, rows, slots * heads, hd), BF16), dma((2,)),
            vmem((2, rows, dim), BF16), dma((2,)),
            vmem((layers, 2, 2 * rows, half), BF16), vmem((2, rows, half), BF16), vmem((rows, half), BF16), dma((2, 2)),
            vmem((2 * rows, group * hd), F32), vmem((2 * rows, 2 * hd), F32),
            vmem((layers, chips, 2, group + 2, rows, hd), BF16), vmem((layers, heads, group + 2, rows, hd), BF16),
            dma((layers, chips)), dma((layers, chips)),
            vmem((layers, chips, 2, group, rows, hd), BF16), dma((layers, chips)), dma((layers, chips)),
            vmem((rows * qh, hd), F32), vmem((rows * qh, hd), F32), vmem((rows * qh, hd), F32),
            vmem((ctx_size, 2 * group * rows, span), F32), vmem((2 * group * rows, ctx_size * span), BF16),
            vmem((layers, chips, 2, group, rows, hd), BF16), vmem((layers, chips, 2, 8, 128), F32),
            vmem((layers, heads, group, rows, hd), BF16), vmem((layers, heads, 8, 128), F32),
            dma((layers, chips, 2)), dma((layers, heads)), dma((layers, chips, 2)), dma((layers, heads)),
            vmem((layers, 2, chips, rows, 2 * group * hd), BF16), dma((layers, chips)), dma((layers, chips)),
            vmem((nblk, 2 * rows, COLS), F32),
        ]
        hid, kvn = pl.pallas_call(
            functools.partial(decode_kernel, ctx_size),
            name="decode",
            out_shape=(jax.ShapeDtypeStruct((2, rows, half), BF16),
                       jax.ShapeDtypeStruct((layers, heads, 2, rows, hd), BF16)),
            in_specs=[spec(memory_space=vmem), spec(memory_space=smem)] + [spec(memory_space=anym)] * 8,
            out_specs=(spec(memory_space=vmem), spec(memory_space=vmem)),
            scratch_shapes=scratch,
            compiler_params=pltpu.CompilerParams(collective_id=0, has_side_effects=True, vmem_limit_bytes=67043328),
        )(hidden, seq_lens, w_query, w_key, w_value, w_out, k_prefix, v_prefix,
          k_suffix.reshape(layers, rows, slots * heads, hd), v_suffix.reshape(layers, rows, slots * heads, hd))
        copies = layers * 2 * (rows // 8)
        return pl.pallas_call(
            cache_kernel,
            name="caches",
            out_shape=(jax.ShapeDtypeStruct(hidden.shape, BF16), jax.ShapeDtypeStruct(k_suffix.shape, BF16),
                       jax.ShapeDtypeStruct(v_suffix.shape, BF16)),
            in_specs=[spec(memory_space=smem), spec(memory_space=vmem), spec(memory_space=vmem),
                      spec(memory_space=anym), spec(memory_space=anym)],
            out_specs=(spec(memory_space=vmem), spec(memory_space=anym), spec(memory_space=anym)),
            scratch_shapes=[vmem((layers, 2, rows, slots, heads, hd), BF16), vmem((layers, 2, rows * heads, hd), F32),
                            dma((copies,)), dma((copies,))],
            compiler_params=pltpu.CompilerParams(vmem_limit_bytes=67043328),
        )(seq_lens, hid, kvn, k_suffix, v_suffix)

    return jax.shard_map(local_step, mesh=mesh,
                         in_specs=(row_spec, lens_spec, whole, whole, whole, whole, prefix_spec, prefix_spec, cache_spec, cache_spec),
                         out_specs=(row_spec, cache_spec, cache_spec), check_vma=False)
```

```python
import functools

import jax
import jax.numpy as jnp
from jax import lax
from jax.experimental import pallas as pl
from jax.experimental.pallas import tpu as pltpu
from jax.sharding import PartitionSpec as P

MESH = pl.DeviceIdType.MESH
BF16 = jnp.bfloat16
F32 = jnp.float32
RING = 10
COLS = 512
LOG2E = 1.4426950408889634
FLOOR = float(jnp.finfo(jnp.float32).min)


def dot(a, b):
    return lax.dot_general(a, b, (((1,), (0,)), ((), ())), preferred_element_type=F32)


def dot_t(a, b):
    return lax.dot_general(a, b, (((1,), (1,)), ((), ())), preferred_element_type=F32)


def decode_kernel(ctx_size, hidden, lens_hbm, wq, wk, wv, wo, kpre, vpre, ksuf, vsuf, hid_out, kvn_out,
                  lens, io_sem, ring, w_sem, wo_buf, wo_sem, pst, pst_sem, pf32, psend, precv, ps_s, ps_r,
                  suf, suf_sem, xh, fin_st, fin_rc, x_sem, acc, qkv_st, hq, hs_s, hs_r,
                  q_rc, q_s, q_r, qs, os, ls, lm, sc, pb, o_st, lse_st, o_rc, lse_rc, o_s, o_r, l_s, l_r,
                  o_cat, oc_s, oc_r, acc_o):
    layers = wq.shape[0]
    dim = wq.shape[1]
    half = dim // 2
    kc = dim // 4
    rows, heads, hd = hidden.shape[0], kpre.shape[2], kpre.shape[3]
    qh = (wq.shape[2] // hd)
    group = wq.shape[2] // (heads * hd)
    span = kpre.shape[1]
    slots = ksuf.shape[2] // heads
    chips = ctx_size // 2
    order = (2, 1, 3, 0)
    scale = hd ** -0.5
    c2 = scale * LOG2E
    gq = group * hd
    nblk = half // COLS

    me = lax.axis_index("ctx")
    chip = me // 2
    core = me % 2
    other = 1 - core
    partner = chip * 2 + other
    pending = []

    def to(dev):
        return {"ctx": dev}

    def remote(src, dst, s_sem, r_sem, dev):
        return pltpu.make_async_remote_copy(src_ref=src, dst_ref=dst, send_sem=s_sem, recv_sem=r_sem,
                                            device_id=to(dev), device_id_type=MESH)

    def send(src, dst, s_sem, r_sem, dev):
        copy = remote(src, dst, s_sem, r_sem, dev)
        copy.start()
        pending.append(copy)

    def arrived(dst, r_sem, s_sem):
        remote(dst, dst, s_sem, r_sem, partner).wait_recv()

    def dest_chip(t):
        return (chip + order[t]) % chips

    def src_chip(t):
        return (chip + chips - order[t]) % chips

    def weight_place(layer, n):
        if layer == 0:
            return n // 4, (n // 2) % 2, n % 2
        return (n // 2) % chips, n // (2 * chips), n % 2

    def weight_copies(layer, n):
        t, hh, kk = weight_place(layer, n)
        slot = (layer * 4 * chips + n) % RING
        g = dest_chip(t) * 2 + core
        krows = pl.ds(pl.multiple_of(((core + hh) % 2) * half + kk * kc, 128), kc)
        qcols = pl.ds(pl.multiple_of(g * gq, gq), gq)
        kcols = pl.ds(pl.multiple_of(g * hd, hd), hd)
        return (
            pltpu.make_async_copy(wq.at[layer, krows, qcols], ring.at[slot, :, 0:gq], w_sem.at[slot, 0]),
            pltpu.make_async_copy(wk.at[layer, krows, kcols], ring.at[slot, :, gq:gq + hd], w_sem.at[slot, 1]),
            pltpu.make_async_copy(wv.at[layer, krows, kcols], ring.at[slot, :, gq + hd:gq + 2 * hd], w_sem.at[slot, 2]),
        )

    def fetch_weights(layer, first, last):
        for n in range(first, min(last, 4 * chips)):
            for copy in weight_copies(layer, n):
                copy.start()

    def wo_copy(layer, tc, nb):
        return pltpu.make_async_copy(
            wo.at[layer, pl.ds(pl.multiple_of(tc * 2 * gq, 2 * gq), 2 * gq),
                  pl.ds(pl.multiple_of(core * half + nb * COLS, COLS), COLS)],
            wo_buf.at[tc, nb], wo_sem.at[tc, nb])

    def fetch_wo(layer, tc):
        for nb in range(nblk):
            wo_copy(layer, tc, nb).start()

    def prefix_copies(layer):
        return (pltpu.make_async_copy(kpre.at[layer], pst.at[0], pst_sem.at[0]),
                pltpu.make_async_copy(vpre.at[layer], pst.at[1], pst_sem.at[1]))

    def suffix_copies(layer):
        return (pltpu.make_async_copy(ksuf.at[layer], suf.at[0], suf_sem.at[0]),
                pltpu.make_async_copy(vsuf.at[layer], suf.at[1], suf_sem.at[1]))

    def relayout_prefix(layer, kv):
        prefix_copies(layer)[kv].wait()
        step = 64

        @pl.loop(0, span // step)
        def _(blk):
            base = pl.multiple_of(blk * step, step)
            pf32[...] = pst[kv, pl.ds(base, step)].astype(F32).reshape(step * heads, hd)
            for g in range(heads):
                psend[layer, g, kv, pl.ds(base, step), :] = pf32[pl.ds(g, step, stride=heads), :].astype(BF16)

    def send_prefix(layer, kv):
        for d in (4, 5, 3, 2, 6, 7, 1):
            dev = (me + d) % ctx_size
            send(psend.at[layer, dev, kv], precv.at[layer, kv, me], ps_s.at[layer, kv, dev], ps_r.at[layer, kv, me], dev)
        precv[layer, kv, me] = psend[layer, me, kv]

    def await_prefix(layer):
        for d in (1, 7, 2, 6, 3, 5, 4):
            src = (me + d) % ctx_size
            for kv in range(2):
                arrived(precv.at[layer, kv, src], ps_r.at[layer, kv, src], ps_s.at[layer, kv, src])

    def dots(layer, chunks):
        for n in chunks:
            for copy in weight_copies(layer, n):
                copy.wait()
        total = None
        for n in chunks:
            _, hh, kk = weight_place(layer, n)
            slot = (layer * 4 * chips + n) % RING
            part = dot(xh[layer, (core + hh) % 2, :, kk * kc:(kk + 1) * kc], ring[slot])
            total = part if total is None else total + part
        return total

    def project(layer, t):
        if layer == 0:
            chunks = range(4 * t, 4 * t + 4)
            total = dots(layer, chunks)
        else:
            chunks = range(2 * chips + 2 * t, 2 * chips + 2 * t + 2)
            total = acc[t] + dots(layer, chunks)
        qkv = total.astype(BF16)
        for n in chunks:
            fetch_weights(layer, n + RING, n + RING + 1)
        if layer == 0 and t >= 2:
            fetch_wo(0, 2 * (t - 2))
            fetch_wo(0, 2 * (t - 2) + 1)

        for cr in range(2):
            part = slice(cr * rows, (cr + 1) * rows)
            for j in range(group):
                qkv_st[layer, t, cr, j] = qkv[part, j * hd:(j + 1) * hd]
            for i in range(2):
                qkv_st[layer, t, cr, group + i] = qkv[part, gq + i * hd:gq + (i + 1) * hd]
        tc = dest_chip(t)
        if order[t] != 0:
            send(qkv_st.at[layer, t, :, 0:group], q_rc.at[layer, chip], q_s.at[layer, t], q_r.at[layer, chip],
                 tc * 2 + core)
        else:
            q_rc[layer, chip] = qkv_st[layer, t, :, 0:group]
        g = tc * 2 + core
        send(qkv_st.at[layer, t, other], hq.at[layer, g], hs_s.at[layer, t], hs_r.at[layer, t], partner)
        hq[layer, g] = qkv_st[layer, t, core]

    def suffix_attention(layer):
        for t in range(chips):
            arrived(hq.at[layer, dest_chip(t) * 2 + other], hs_r.at[layer, t], hs_s.at[layer, t])
        for g in range(heads):
            for j in range(group):
                qs[pl.ds(g * group + j, rows, stride=heads * group), :] = hq[layer, g, j].astype(F32)
        for copy in suffix_copies(layer):
            copy.wait()
        row_id = lax.broadcasted_iota(jnp.int32, (qh, slots * heads), 0)
        col_id = lax.broadcasted_iota(jnp.int32, (qh, slots * heads), 1)
        slot_of = jnp.where((row_id // group) == (col_id % heads), col_id // heads, slots)
        step = 8

        @pl.loop(0, rows // step)
        def _(blk):
            for i in range(step):
                b = blk * step + i
                base = pl.multiple_of(b * qh, qh)
                s = dot_t(qs[pl.ds(base, qh), :].astype(BF16), suf[0, b])
                s = jnp.where(slot_of < lens[b], s, FLOOR)
                m = jnp.max(s, axis=1, keepdims=True)
                e = jnp.exp2((s - m) * c2)
                mass = jnp.sum(e, axis=1, keepdims=True)
                val = dot(e.astype(BF16), suf[1, b])
                os[pl.ds(base, qh), :] = val * (1.0 / mass)
                ls[pl.ds(base, qh), :] = jnp.broadcast_to(m * scale + jnp.log(mass), (qh, hd))

        for g in range(heads):
            k_new = hq[layer, g, group].astype(F32)
            v_new = hq[layer, g, group + 1].astype(F32)
            for j in range(group):
                h = g * group + j
                picked = pl.ds(h, rows, stride=qh)
                lo = ls[picked, :]
                sn = jnp.sum(hq[layer, g, j].astype(F32) * k_new, axis=1, keepdims=True) * scale
                top = jnp.maximum(lo, sn)
                w_old = jnp.exp(lo - top)
                w_new = jnp.exp(sn - top)
                mass = w_old + w_new
                qs[h * rows:(h + 1) * rows, :] = (w_old * os[picked, :] + w_new * v_new) / mass
                lm[h * rows:(h + 1) * rows, :] = top + jnp.log(mass)

    def prefix_attention(layer, t):
        src = src_chip(t)
        if order[t] != 0:
            arrived(q_rc.at[layer, src], q_r.at[layer, src], q_s.at[layer, t])
        q = q_rc[layer, src].reshape(2 * group * rows, hd)
        peak = None
        for s in range(ctx_size):
            part = dot_t(q, precv[layer, 0, s])
            sc[s] = part
            for lo in range(0, span, 128):
                piece = part[:, lo:lo + 128]
                peak = piece if peak is None else jnp.maximum(peak, piece)
        m = jnp.max(peak, axis=1, keepdims=True)
        mass = jnp.zeros((2 * group * rows, 128), F32)
        for s in range(ctx_size):
            e = jnp.exp2((sc[s] - m) * c2)
            for lo in range(0, span, 128):
                mass = mass + e[:, lo:lo + 128]
            pb[:, s * span:(s + 1) * span] = e.astype(BF16)
        mass = jnp.sum(mass, axis=1, keepdims=True)
        vals = dot(pb[...], precv[layer, 1].reshape(ctx_size * span, hd))
        out = (vals * (1.0 / mass)).astype(BF16)
        lse = jnp.broadcast_to(m * scale + jnp.log(mass), (2 * group * rows, 128)).T
        for cr in range(2):
            part = group * rows
            o_st[layer, t, cr] = out[cr * part:(cr + 1) * part].reshape(group, rows, hd)
            lse_st[layer, t, cr] = lse[0:8, cr * part:(cr + 1) * part]
        if order[t] != 0:
            for cr in range(2):
                dev = src * 2 + cr
                send(lse_st.at[layer, t, cr], lse_rc.at[layer, me], l_s.at[layer, t, cr], l_r.at[layer, me], dev)
                send(o_st.at[layer, t, cr], o_rc.at[layer, me], o_s.at[layer, t, cr], o_r.at[layer, me], dev)
        else:
            send(lse_st.at[layer, t, other], lse_rc.at[layer, me], l_s.at[layer, t, 0], l_r.at[layer, me], partner)
            send(o_st.at[layer, t, other], o_rc.at[layer, me], o_s.at[layer, t, 0], o_r.at[layer, me], partner)
            lse_rc[layer, me] = lse_st[layer, t, core]
            o_rc[layer, me] = o_st[layer, t, core]

    def combine(layer, t):
        tc = dest_chip(t)
        for par in range(2):
            if order[t] != 0:
                g = tc * 2 + par
                arrived(lse_rc.at[layer, g], l_r.at[layer, g], l_s.at[layer, t, 0])
                arrived(o_rc.at[layer, g], o_r.at[layer, g], o_s.at[layer, t, 0])
            elif par == 0:
                arrived(lse_rc.at[layer, partner], l_r.at[layer, partner], l_s.at[layer, t, 0])
                arrived(o_rc.at[layer, partner], o_r.at[layer, partner], o_s.at[layer, t, 0])
        for par in range(2):
            g = tc * 2 + par
            lse_p = jnp.broadcast_to(lse_rc[layer, g, 0:1, :], (group * rows, 128)).T
            for j in range(group):
                here = pl.ds(pl.multiple_of((g * group + j) * rows, rows), rows)
                lp = lse_p[j * rows:(j + 1) * rows]
                lo = lm[here, :]
                top = jnp.maximum(lp, lo)
                wp = jnp.exp(lp - top)
                ws = jnp.exp(lo - top)
                mixed = wp * o_rc[layer, g, j].astype(F32) + ws * qs[here, :]
                at = (par * group + j) * hd
                o_cat[layer, core, tc, :, at:at + hd] = (mixed / (wp + ws)).astype(BF16)
        send(o_cat.at[layer, core, tc], o_cat.at[layer, core, tc], oc_s.at[layer, t], oc_r.at[layer, t], partner)

    def project_out(layer, t):
        tc = dest_chip(t)
        arrived(o_cat.at[layer, other, tc], oc_r.at[layer, t], oc_s.at[layer, t])
        lhs = jnp.concatenate([o_cat[layer, 0, tc], o_cat[layer, 1, tc]], axis=0)

        for nb in range(nblk):
            wo_copy(layer, tc, nb).wait()
        for nb in range(nblk):
            upd = dot(lhs, wo_buf[tc, nb])
            if t == 0:
                acc_o[nb] = upd
            else:
                acc_o[nb] += upd
            if layer + 1 < layers:
                wo_copy(layer + 1, tc, nb).start()

    own = pl.ds(pl.multiple_of(core * rows, rows), rows)
    theirs = pl.ds(pl.multiple_of(other * rows, rows), rows)
    for copy in prefix_copies(0):
        copy.start()
    loads = [pltpu.make_async_copy(lens_hbm, lens, io_sem.at[0])]
    for sd in range(2):
        loads.append(pltpu.make_async_copy(hidden.at[:, sd * half:(sd + 1) * half], xh.at[0, sd, own, :], io_sem.at[1 + sd]))
    for copy in loads:
        copy.start()
    fetch_weights(0, 0, RING)
    barrier = pltpu.get_barrier_semaphore()
    for d in range(1, ctx_size):
        pl.semaphore_signal(barrier, inc=1, device_id=to((me + d) % ctx_size), device_id_type=MESH)
    relayout_prefix(0, 0)
    for copy in loads:
        copy.wait()
    pl.semaphore_wait(barrier, ctx_size - 1)
    send(xh.at[0, :, own, :], xh.at[0, :, own, :], x_sem.at[2, 0], x_sem.at[2, 1], partner)
    send_prefix(0, 0)
    relayout_prefix(0, 1)
    send_prefix(0, 1)
    arrived(xh.at[0, :, theirs, :], x_sem.at[2, 1], x_sem.at[2, 0])

    for layer in range(layers):
        if layer > 0:
            for t in range(chips):
                acc[t] = dots(layer, (2 * t, 2 * t + 1))
                for n in (2 * t, 2 * t + 1):
                    fetch_weights(layer, n + RING, n + RING + 1)
            arrived(xh.at[layer, other], x_sem.at[0, 1], x_sem.at[0, 0])
        for t in range(chips):
            project(layer, t)
            if layer == 0 and t == 1:
                for copy in suffix_copies(0):
                    copy.start()
        if layer + 1 < layers:
            for copy in prefix_copies(layer + 1):
                copy.start()
            fetch_weights(layer + 1, 0, RING)
            suffix_attention(layer)
            for copy in suffix_copies(layer + 1):
                copy.start()
            for kv in range(2):
                relayout_prefix(layer + 1, kv)
            await_prefix(layer)
            for t in range(chips):
                prefix_attention(layer, t)
            for kv in range(2):
                send_prefix(layer + 1, kv)
        else:
            await_prefix(layer)
            for t in (3, 0, 1, 2):
                prefix_attention(layer, t)
            suffix_attention(layer)
        for t in range(chips):
            combine(layer, t)
            if t > 0:
                project_out(layer, t - 1)
        project_out(layer, chips - 1)
        for nb in range(nblk):
            cols = slice(nb * COLS, (nb + 1) * COLS)
            new = (xh[layer, core, :, cols].astype(F32) + acc_o[nb].astype(BF16).astype(F32)).astype(BF16)
            if layer + 1 < layers:
                xh[layer + 1, core, :, cols] = new
            else:
                for cr in range(2):
                    fin_st[cr, :, cols] = new[cr * rows:(cr + 1) * rows]
        if layer + 1 < layers:
            send(xh.at[layer + 1, core], xh.at[layer + 1, core], x_sem.at[0, 0], x_sem.at[0, 1], partner)
    send(fin_st.at[other], fin_rc, x_sem.at[1, 0], x_sem.at[1, 1], partner)
    stores = [pltpu.make_async_copy(fin_st.at[core], hid_out.at[core], io_sem.at[0]),
              pltpu.make_async_copy(hq.at[:, :, group:group + 2], kvn_out, io_sem.at[1])]
    for copy in stores:
        copy.start()
    arrived(fin_rc, x_sem.at[1, 1], x_sem.at[1, 0])
    stores.append(pltpu.make_async_copy(fin_rc, hid_out.at[other], io_sem.at[2]))
    stores[2].start()
    for copy in stores:
        copy.wait()
    for copy in pending:
        copy.wait_send()


def cache_kernel(lens, hid, kvn, ksuf, vsuf, hid_out, kout, vout, buf, tiles, hbuf, kvbuf, in_sem, out_sem, io_sem):
    layers, batch = ksuf.shape[0], ksuf.shape[1]
    heads = ksuf.shape[3]
    half = hid.shape[2]
    step = 8
    parts = batch // step
    srcs, dsts = (ksuf, vsuf), (kout, vout)

    def copies(layer, i, part, out):
        here = pl.ds(part * step, step)
        at = (layer * 2 + i) * parts + part
        if out:
            return pltpu.make_async_copy(buf.at[layer, i, here], dsts[i].at[layer, here], out_sem.at[at])
        return pltpu.make_async_copy(srcs[i].at[layer, here], buf.at[layer, i, here], in_sem.at[at])

    todo = [(layer, i, part) for layer in range(layers) for i in range(2) for part in range(parts)]
    news = pltpu.make_async_copy(kvn, kvbuf, io_sem.at[0])
    news.start()
    for layer, i, part in todo:
        copies(layer, i, part, False).start()
    sides = [pltpu.make_async_copy(hid.at[sd], hbuf.at[:, sd * half:(sd + 1) * half], io_sem.at[1 + sd]) for sd in range(2)]
    for copy in sides:
        copy.start()
    news.wait()
    for layer in range(layers):
        for i in range(2):
            for g in range(heads):
                tiles[layer, i, pl.ds(g, batch, stride=heads), :] = kvbuf[layer, g, i].astype(F32)
    for layer, i, part in todo:
        copies(layer, i, part, False).wait()
        for b in range(part * step, (part + 1) * step):
            buf[layer, i, b, lens[b]] = tiles[layer, i, b * heads:(b + 1) * heads, :].astype(BF16)
        copies(layer, i, part, True).start()
    for copy in sides:
        copy.wait()
    whole = pltpu.make_async_copy(hbuf, hid_out, io_sem.at[3])
    whole.start()
    for layer, i, part in todo:
        copies(layer, i, part, True).wait()
    whole.wait()


def solution(mesh):
    ctx_size = mesh.shape["ctx"]
    home = ("data", "ctx")
    row_spec, lens_spec, whole = P(home, None), P(home), P()
    prefix_spec = P(None, home, None, None)
    cache_spec = P(None, home, None, None, None)

    def local_step(hidden, seq_lens, w_query, w_key, w_value, w_out, k_prefix, v_prefix, k_suffix, v_suffix):
        layers, dim, q_width = w_query.shape
        rows = hidden.shape[0]
        span, heads, hd = k_prefix.shape[1:]
        slots = k_suffix.shape[2]
        group = q_width // (heads * hd)
        chips = ctx_size // 2
        half, kc = dim // 2, dim // 4
        nblk = half // COLS
        qh = heads * group
        vmem, smem, anym = pltpu.VMEM, pltpu.SMEM, pl.ANY
        dma = pltpu.SemaphoreType.DMA
        spec = pl.BlockSpec
        scratch = [
            smem((rows,), jnp.int32), dma((3,)),
            vmem((RING, kc, (group + 2) * hd), BF16), dma((RING, 3)),
            vmem((chips, nblk, 2 * group * hd, COLS), BF16), dma((chips, nblk)),
            vmem((2, span, heads, hd), BF16), dma((2,)), vmem((64 * heads, hd), F32),
            vmem((layers, ctx_size, 2, span, hd), BF16), vmem((layers, 2, ctx_size, span, hd), BF16),
            dma((layers, 2, ctx_size)), dma((layers, 2, ctx_size)),
            vmem((2, rows, slots * heads, hd), BF16), dma((2,)),
            vmem((layers, 2, 2 * rows, half), BF16), vmem((2, rows, half), BF16), vmem((rows, half), BF16), dma((3, 2)),
            vmem((chips, 2 * rows, (group + 2) * hd), F32),
            vmem((layers, chips, 2, group + 2, rows, hd), BF16), vmem((layers, heads, group + 2, rows, hd), BF16),
            dma((layers, chips)), dma((layers, chips)),
            vmem((layers, chips, 2, group, rows, hd), BF16), dma((layers, chips)), dma((layers, chips)),
            vmem((rows * qh, hd), F32), vmem((rows * qh, hd), F32), vmem((rows * qh, hd), F32), vmem((rows * qh, hd), F32),
            vmem((ctx_size, 2 * group * rows, span), F32), vmem((2 * group * rows, ctx_size * span), BF16),
            vmem((layers, chips, 2, group, rows, hd), BF16), vmem((layers, chips, 2, 8, 128), F32),
            vmem((layers, heads, group, rows, hd), BF16), vmem((layers, heads, 8, 128), F32),
            dma((layers, chips, 2)), dma((layers, heads)), dma((layers, chips, 2)), dma((layers, heads)),
            vmem((layers, 2, chips, rows, 2 * group * hd), BF16), dma((layers, chips)), dma((layers, chips)),
            vmem((nblk, 2 * rows, COLS), F32),
        ]
        hid, kvn = pl.pallas_call(
            functools.partial(decode_kernel, ctx_size),
            name="decode",
            out_shape=(jax.ShapeDtypeStruct((2, rows, half), BF16),
                       jax.ShapeDtypeStruct((layers, heads, 2, rows, hd), BF16)),
            in_specs=[spec(memory_space=anym)] * 10,
            out_specs=(spec(memory_space=anym), spec(memory_space=anym)),
            scratch_shapes=scratch,
            compiler_params=pltpu.CompilerParams(collective_id=0, has_side_effects=True, vmem_limit_bytes=67043328),
        )(hidden, seq_lens, w_query, w_key, w_value, w_out, k_prefix, v_prefix,
          k_suffix.reshape(layers, rows, slots * heads, hd), v_suffix.reshape(layers, rows, slots * heads, hd))
        copies = layers * 2 * (rows // 8)
        return pl.pallas_call(
            cache_kernel,
            name="caches",
            out_shape=(jax.ShapeDtypeStruct(hidden.shape, BF16), jax.ShapeDtypeStruct(k_suffix.shape, BF16),
                       jax.ShapeDtypeStruct(v_suffix.shape, BF16)),
            in_specs=[spec(memory_space=smem)] + [spec(memory_space=anym)] * 4,
            out_specs=(spec(memory_space=anym), spec(memory_space=anym), spec(memory_space=anym)),
            scratch_shapes=[vmem((layers, 2, rows, slots, heads, hd), BF16), vmem((layers, 2, rows * heads, hd), F32),
                            vmem((rows, dim), BF16), vmem((layers, heads, 2, rows, hd), BF16),
                            dma((copies,)), dma((copies,)), dma((4,))],
            compiler_params=pltpu.CompilerParams(vmem_limit_bytes=67043328),
        )(seq_lens, hid, kvn, k_suffix, v_suffix)

    return jax.shard_map(local_step, mesh=mesh,
                         in_specs=(row_spec, lens_spec, whole, whole, whole, whole, prefix_spec, prefix_spec, cache_spec, cache_spec),
                         out_specs=(row_spec, cache_spec, cache_spec), check_vma=False)
```

```python
import functools

import jax
import jax.numpy as jnp
from jax import lax
from jax.experimental import pallas as pl
from jax.experimental.pallas import tpu as pltpu
from jax.sharding import PartitionSpec as P

MESH = pl.DeviceIdType.MESH
BF16 = jnp.bfloat16
F32 = jnp.float32
RING = 10
COLS = 512
PAD = 8
LOG2E = 1.4426950408889634
FLOOR = float(jnp.finfo(jnp.float32).min)


def dot(a, b):
    return lax.dot_general(a, b, (((1,), (0,)), ((), ())), preferred_element_type=F32)


def dot_t(a, b):
    return lax.dot_general(a, b, (((1,), (1,)), ((), ())), preferred_element_type=F32)


def decode_kernel(ctx_size, hidden, lens_hbm, wq, wk, wv, wo, kpre, vpre, ksuf, vsuf, hid_out, kvn_out,
                  lens, io_sem, ring, w_sem, wo_buf, wo_sem, pst, pst_sem, pf32, psend, precv, ps_s, ps_r,
                  suf, suf_sem, xh, fin_st, fin_rc, x_sem, acc, qkv_st, hq, hs_s, hs_r,
                  q_rc, q_s, q_r, qs, os, ls, lm, sc, pb, o_st, lse_st, o_rc, lse_rc, o_s, o_r, l_s, l_r,
                  o_cat, oc_s, oc_r, acc_o):
    layers = wq.shape[0]
    dim = wq.shape[1]
    half = dim // 2
    kc = dim // 4
    rows, heads, hd = hidden.shape[0], kpre.shape[2], kpre.shape[3]
    qh = (wq.shape[2] // hd)
    group = wq.shape[2] // (heads * hd)
    span = kpre.shape[1]
    slots = ksuf.shape[2] // heads
    chips = ctx_size // 2
    order = (2, 1, 3, 0)
    scale = hd ** -0.5
    c2 = scale * LOG2E
    gq = group * hd
    nblk = half // COLS
    pitch = qh + PAD

    me = lax.axis_index("ctx")
    chip = me // 2
    core = me % 2
    other = 1 - core
    partner = chip * 2 + other
    pending = []

    def to(dev):
        return {"ctx": dev}

    def remote(src, dst, s_sem, r_sem, dev):
        return pltpu.make_async_remote_copy(src_ref=src, dst_ref=dst, send_sem=s_sem, recv_sem=r_sem,
                                            device_id=to(dev), device_id_type=MESH)

    def send(src, dst, s_sem, r_sem, dev):
        copy = remote(src, dst, s_sem, r_sem, dev)
        copy.start()
        pending.append(copy)

    def arrived(dst, r_sem, s_sem):
        remote(dst, dst, s_sem, r_sem, partner).wait_recv()

    def dest_chip(t):
        return (chip + order[t]) % chips

    def src_chip(t):
        return (chip + chips - order[t]) % chips

    def weight_place(layer, n):
        if layer == 0:
            return n // 4, (n // 2) % 2, n % 2
        return (n // 2) % chips, n // (2 * chips), n % 2

    def weight_copies(layer, n):
        t, hh, kk = weight_place(layer, n)
        slot = (layer * 4 * chips + n) % RING
        g = dest_chip(t) * 2 + core
        krows = pl.ds(pl.multiple_of(((core + hh) % 2) * half + kk * kc, 128), kc)
        qcols = pl.ds(pl.multiple_of(g * gq, gq), gq)
        kcols = pl.ds(pl.multiple_of(g * hd, hd), hd)
        return (
            pltpu.make_async_copy(wq.at[layer, krows, qcols], ring.at[slot, :, 0:gq], w_sem.at[slot, 0]),
            pltpu.make_async_copy(wk.at[layer, krows, kcols], ring.at[slot, :, gq:gq + hd], w_sem.at[slot, 1]),
            pltpu.make_async_copy(wv.at[layer, krows, kcols], ring.at[slot, :, gq + hd:gq + 2 * hd], w_sem.at[slot, 2]),
        )

    def fetch_weights(layer, first, last):
        for n in range(first, min(last, 4 * chips)):
            for copy in weight_copies(layer, n):
                copy.start()

    def wo_copy(layer, tc, nb):
        return pltpu.make_async_copy(
            wo.at[layer, pl.ds(pl.multiple_of(tc * 2 * gq, 2 * gq), 2 * gq),
                  pl.ds(pl.multiple_of(core * half + nb * COLS, COLS), COLS)],
            wo_buf.at[tc, nb], wo_sem.at[tc, nb])

    def fetch_wo(layer, tc):
        for nb in range(nblk):
            wo_copy(layer, tc, nb).start()

    def prefix_copies(layer):
        return (pltpu.make_async_copy(kpre.at[layer], pst.at[0], pst_sem.at[0]),
                pltpu.make_async_copy(vpre.at[layer], pst.at[1], pst_sem.at[1]))

    def suffix_copies(layer):
        return (pltpu.make_async_copy(ksuf.at[layer], suf.at[0], suf_sem.at[0]),
                pltpu.make_async_copy(vsuf.at[layer], suf.at[1], suf_sem.at[1]))

    def relayout_prefix(layer, kv):
        prefix_copies(layer)[kv].wait()
        step = 64

        @pl.loop(0, span // step)
        def _(blk):
            base = pl.multiple_of(blk * step, step)
            pf32[...] = pst[kv, pl.ds(base, step)].astype(F32).reshape(step * heads, hd)
            for g in range(heads):
                psend[layer, g, kv, pl.ds(base, step), :] = pf32[pl.ds(g, step, stride=heads), :].astype(BF16)

    def send_prefix(layer, kv):
        for d in (4, 5, 3, 2, 6, 7, 1):
            dev = (me + d) % ctx_size
            send(psend.at[layer, dev, kv], precv.at[layer, kv, me], ps_s.at[layer, kv, dev], ps_r.at[layer, kv, me], dev)
        precv[layer, kv, me] = psend[layer, me, kv]

    def await_prefix(layer):
        for d in (1, 7, 2, 6, 3, 5, 4):
            src = (me + d) % ctx_size
            for kv in range(2):
                arrived(precv.at[layer, kv, src], ps_r.at[layer, kv, src], ps_s.at[layer, kv, src])

    def dots(layer, chunks):
        for n in chunks:
            for copy in weight_copies(layer, n):
                copy.wait()
        total = None
        for n in chunks:
            _, hh, kk = weight_place(layer, n)
            slot = (layer * 4 * chips + n) % RING
            part = dot(xh[layer, (core + hh) % 2, :, kk * kc:(kk + 1) * kc], ring[slot])
            total = part if total is None else total + part
        return total

    def project(layer, t):
        if layer == 0:
            chunks = range(4 * t, 4 * t + 4)
            total = dots(layer, chunks)
        else:
            chunks = range(2 * chips + 2 * t, 2 * chips + 2 * t + 2)
            total = acc[t] + dots(layer, chunks)
        qkv = total.astype(BF16)
        for n in chunks:
            fetch_weights(layer, n + RING, n + RING + 1)
        if layer == 0 and t >= 2:
            fetch_wo(0, 2 * (t - 2))
            fetch_wo(0, 2 * (t - 2) + 1)

        for cr in range(2):
            part = slice(cr * rows, (cr + 1) * rows)
            for j in range(group):
                qkv_st[layer, t, cr, j] = qkv[part, j * hd:(j + 1) * hd]
            for i in range(2):
                qkv_st[layer, t, cr, group + i] = qkv[part, gq + i * hd:gq + (i + 1) * hd]
        tc = dest_chip(t)
        if order[t] != 0:
            send(qkv_st.at[layer, t, :, 0:group], q_rc.at[layer, chip], q_s.at[layer, t], q_r.at[layer, chip],
                 tc * 2 + core)
        else:
            q_rc[layer, chip] = qkv_st[layer, t, :, 0:group]
        g = tc * 2 + core
        send(qkv_st.at[layer, t, other], hq.at[layer, g], hs_s.at[layer, t], hs_r.at[layer, t], partner)
        hq[layer, g] = qkv_st[layer, t, core]

    def suffix_queries(layer):
        for t in range(chips):
            arrived(hq.at[layer, dest_chip(t) * 2 + other], hs_r.at[layer, t], hs_s.at[layer, t])
        for g in range(heads):
            for j in range(group):
                qs[pl.ds(g * group + j, rows, stride=pitch), :] = hq[layer, g, j].astype(F32)
        for copy in suffix_copies(layer):
            copy.wait()

    def suffix_attention(layer, first, last):
        row_id = lax.broadcasted_iota(jnp.int32, (qh, slots * heads), 0)
        col_id = lax.broadcasted_iota(jnp.int32, (qh, slots * heads), 1)
        slot_of = jnp.where((row_id // group) == (col_id % heads), col_id // heads, slots)
        step = 8

        @pl.loop(first // step, last // step)
        def _(blk):
            for i in range(step):
                b = blk * step + i
                base = pl.multiple_of(b * pitch, 8)
                s = dot_t(qs[pl.ds(base, qh), :].astype(BF16), suf[0, b])
                s = jnp.where(slot_of < lens[b], s, FLOOR)
                m = jnp.max(s, axis=1, keepdims=True)
                e = jnp.exp2((s - m) * c2)
                mass = jnp.sum(e, axis=1, keepdims=True)
                val = dot(e.astype(BF16), suf[1, b])
                os[pl.ds(base, qh), :] = val * (1.0 / mass)
                ls[pl.ds(base, qh), :] = jnp.broadcast_to(m * scale + jnp.log(mass), (qh, hd))

    def suffix_merge(layer):
        for g in range(heads):
            k_new = hq[layer, g, group].astype(F32)
            v_new = hq[layer, g, group + 1].astype(F32)
            for j in range(group):
                h = g * group + j
                picked = pl.ds(h, rows, stride=pitch)
                lo = ls[picked, :]
                sn = jnp.sum(hq[layer, g, j].astype(F32) * k_new, axis=1, keepdims=True) * scale
                top = jnp.maximum(lo, sn)
                w_old = jnp.exp(lo - top)
                w_new = jnp.exp(sn - top)
                mass = w_old + w_new
                qs[h * rows:(h + 1) * rows, :] = (w_old * os[picked, :] + w_new * v_new) / mass
                lm[h * rows:(h + 1) * rows, :] = top + jnp.log(mass)

    def prefix_attention(layer, t):
        src = src_chip(t)
        if order[t] != 0:
            arrived(q_rc.at[layer, src], q_r.at[layer, src], q_s.at[layer, t])
        q = q_rc[layer, src].reshape(2 * group * rows, hd)
        peak = None
        for s in range(ctx_size):
            part = dot_t(q, precv[layer, 0, s])
            sc[s] = part
            for lo in range(0, span, 128):
                piece = part[:, lo:lo + 128]
                peak = piece if peak is None else jnp.maximum(peak, piece)
        m = jnp.max(peak, axis=1, keepdims=True)
        mass = jnp.zeros((2 * group * rows, 128), F32)
        for s in range(ctx_size):
            e = jnp.exp2((sc[s] - m) * c2)
            for lo in range(0, span, 128):
                mass = mass + e[:, lo:lo + 128]
            pb[:, s * span:(s + 1) * span] = e.astype(BF16)
        mass = jnp.sum(mass, axis=1, keepdims=True)
        vals = dot(pb[...], precv[layer, 1].reshape(ctx_size * span, hd))
        out = (vals * (1.0 / mass)).astype(BF16)
        lse = jnp.broadcast_to(m * scale + jnp.log(mass), (2 * group * rows, 128)).T
        for cr in range(2):
            part = group * rows
            o_st[layer, t, cr] = out[cr * part:(cr + 1) * part].reshape(group, rows, hd)
            lse_st[layer, t, cr] = lse[0:8, cr * part:(cr + 1) * part]
        if order[t] != 0:
            for cr in range(2):
                dev = src * 2 + cr
                send(lse_st.at[layer, t, cr], lse_rc.at[layer, me], l_s.at[layer, t, cr], l_r.at[layer, me], dev)
                send(o_st.at[layer, t, cr], o_rc.at[layer, me], o_s.at[layer, t, cr], o_r.at[layer, me], dev)
        else:
            send(lse_st.at[layer, t, other], lse_rc.at[layer, me], l_s.at[layer, t, 0], l_r.at[layer, me], partner)
            send(o_st.at[layer, t, other], o_rc.at[layer, me], o_s.at[layer, t, 0], o_r.at[layer, me], partner)
            lse_rc[layer, me] = lse_st[layer, t, core]
            o_rc[layer, me] = o_st[layer, t, core]

    def combine(layer, t):
        tc = dest_chip(t)
        for par in range(2):
            if order[t] != 0:
                g = tc * 2 + par
                arrived(lse_rc.at[layer, g], l_r.at[layer, g], l_s.at[layer, t, 0])
                arrived(o_rc.at[layer, g], o_r.at[layer, g], o_s.at[layer, t, 0])
            elif par == 0:
                arrived(lse_rc.at[layer, partner], l_r.at[layer, partner], l_s.at[layer, t, 0])
                arrived(o_rc.at[layer, partner], o_r.at[layer, partner], o_s.at[layer, t, 0])
        for par in range(2):
            g = tc * 2 + par
            lse_p = jnp.broadcast_to(lse_rc[layer, g, 0:1, :], (group * rows, 128)).T
            for j in range(group):
                here = pl.ds(pl.multiple_of((g * group + j) * rows, rows), rows)
                lp = lse_p[j * rows:(j + 1) * rows]
                lo = lm[here, :]
                top = jnp.maximum(lp, lo)
                wp = jnp.exp(lp - top)
                ws = jnp.exp(lo - top)
                mixed = wp * o_rc[layer, g, j].astype(F32) + ws * qs[here, :]
                at = (par * group + j) * hd
                o_cat[layer, core, tc, :, at:at + hd] = (mixed / (wp + ws)).astype(BF16)
        send(o_cat.at[layer, core, tc], o_cat.at[layer, core, tc], oc_s.at[layer, t], oc_r.at[layer, t], partner)

    def project_out(layer, t):
        tc = dest_chip(t)
        arrived(o_cat.at[layer, other, tc], oc_r.at[layer, t], oc_s.at[layer, t])
        lhs = jnp.concatenate([o_cat[layer, 0, tc], o_cat[layer, 1, tc]], axis=0)

        for nb in range(nblk):
            wo_copy(layer, tc, nb).wait()
        for nb in range(nblk):
            upd = dot(lhs, wo_buf[tc, nb])
            if t == 0:
                acc_o[nb] = upd
            else:
                acc_o[nb] += upd
            if layer + 1 < layers:
                wo_copy(layer + 1, tc, nb).start()

    own = pl.ds(pl.multiple_of(core * rows, rows), rows)
    theirs = pl.ds(pl.multiple_of(other * rows, rows), rows)
    for copy in prefix_copies(0):
        copy.start()
    loads = [pltpu.make_async_copy(lens_hbm, lens, io_sem.at[0])]
    for sd in range(2):
        loads.append(pltpu.make_async_copy(hidden.at[:, sd * half:(sd + 1) * half], xh.at[0, sd, own, :], io_sem.at[1 + sd]))
    for copy in loads:
        copy.start()
    fetch_weights(0, 0, RING)
    barrier = pltpu.get_barrier_semaphore()
    for d in range(1, ctx_size):
        pl.semaphore_signal(barrier, inc=1, device_id=to((me + d) % ctx_size), device_id_type=MESH)
    relayout_prefix(0, 0)
    for copy in loads:
        copy.wait()
    pl.semaphore_wait(barrier, ctx_size - 1)
    send(xh.at[0, :, own, :], xh.at[0, :, own, :], x_sem.at[2, 0], x_sem.at[2, 1], partner)
    send_prefix(0, 0)
    relayout_prefix(0, 1)
    send_prefix(0, 1)
    arrived(xh.at[0, :, theirs, :], x_sem.at[2, 1], x_sem.at[2, 0])

    for layer in range(layers):
        if layer > 0:
            for t in range(chips):
                acc[t] = dots(layer, (2 * t, 2 * t + 1))
                for n in (2 * t, 2 * t + 1):
                    fetch_weights(layer, n + RING, n + RING + 1)
            arrived(xh.at[layer, other], x_sem.at[0, 1], x_sem.at[0, 0])
        for t in range(chips):
            project(layer, t)
            if layer == 0 and t == 1:
                for copy in suffix_copies(0) + prefix_copies(1):
                    copy.start()
        if layer + 1 < layers:
            fetch_weights(layer + 1, 0, RING)
            relayout_prefix(layer + 1, 0)
            send_prefix(layer + 1, 0)
            suffix_queries(layer)
            suffix_attention(layer, 0, rows)
            suffix_merge(layer)
            for copy in suffix_copies(layer + 1):
                copy.start()
            relayout_prefix(layer + 1, 1)
            await_prefix(layer)
            for t in range(chips):
                prefix_attention(layer, t)
            send_prefix(layer + 1, 1)
        else:
            await_prefix(layer)
            prefix_attention(layer, chips - 1)
            suffix_queries(layer)
            suffix_attention(layer, 0, rows // 2)
            for t in range(chips - 1):
                prefix_attention(layer, t)
            suffix_attention(layer, rows // 2, rows)
            suffix_merge(layer)
        for t in range(chips):
            combine(layer, t)
            if t > 0:
                project_out(layer, t - 1)
        project_out(layer, chips - 1)
        for nb in range(nblk):
            cols = slice(nb * COLS, (nb + 1) * COLS)
            new = (xh[layer, core, :, cols].astype(F32) + acc_o[nb].astype(BF16).astype(F32)).astype(BF16)
            if layer + 1 < layers:
                xh[layer + 1, core, :, cols] = new
            else:
                for cr in range(2):
                    fin_st[cr, :, cols] = new[cr * rows:(cr + 1) * rows]
        if layer + 1 < layers:
            send(xh.at[layer + 1, core], xh.at[layer + 1, core], x_sem.at[0, 0], x_sem.at[0, 1], partner)
    send(fin_st.at[other], fin_rc, x_sem.at[1, 0], x_sem.at[1, 1], partner)
    stores = [pltpu.make_async_copy(fin_st.at[core], hid_out.at[core], io_sem.at[0]),
              pltpu.make_async_copy(hq.at[:, :, group:group + 2], kvn_out, io_sem.at[1])]
    for copy in stores:
        copy.start()
    arrived(fin_rc, x_sem.at[1, 1], x_sem.at[1, 0])
    stores.append(pltpu.make_async_copy(fin_rc, hid_out.at[other], io_sem.at[2]))
    stores[2].start()
    for copy in stores:
        copy.wait()
    for copy in pending:
        copy.wait_send()


def cache_kernel(lens, hid, kvn, ksuf, vsuf, hid_out, kout, vout, buf, tiles, hbuf, kvbuf, in_sem, out_sem, io_sem):
    layers, batch = ksuf.shape[0], ksuf.shape[1]
    heads = ksuf.shape[3]
    half = hid.shape[2]
    step = 8
    parts = batch // step
    srcs, dsts = (ksuf, vsuf), (kout, vout)

    def copies(layer, i, part, out):
        here = pl.ds(part * step, step)
        at = (layer * 2 + i) * parts + part
        if out:
            return pltpu.make_async_copy(buf.at[layer, i, here], dsts[i].at[layer, here], out_sem.at[at])
        return pltpu.make_async_copy(srcs[i].at[layer, here], buf.at[layer, i, here], in_sem.at[at])

    todo = [(layer, i, part) for layer in range(layers) for i in range(2) for part in range(parts)]
    news = pltpu.make_async_copy(kvn, kvbuf, io_sem.at[0])
    news.start()
    for layer, i, part in todo:
        copies(layer, i, part, False).start()
    sides = [pltpu.make_async_copy(hid.at[sd], hbuf.at[:, sd * half:(sd + 1) * half], io_sem.at[1 + sd]) for sd in range(2)]
    for copy in sides:
        copy.start()
    news.wait()
    for layer in range(layers):
        for i in range(2):
            for g in range(heads):
                tiles[layer, i, pl.ds(g, batch, stride=heads), :] = kvbuf[layer, g, i].astype(F32)
    for layer, i, part in todo:
        copies(layer, i, part, False).wait()
        for b in range(part * step, (part + 1) * step):
            buf[layer, i, b, lens[b]] = tiles[layer, i, b * heads:(b + 1) * heads, :].astype(BF16)
        copies(layer, i, part, True).start()
    for copy in sides:
        copy.wait()
    whole = pltpu.make_async_copy(hbuf, hid_out, io_sem.at[3])
    whole.start()
    for layer, i, part in todo:
        copies(layer, i, part, True).wait()
    whole.wait()


def solution(mesh):
    ctx_size = mesh.shape["ctx"]
    home = ("data", "ctx")
    row_spec, lens_spec, whole = P(home, None), P(home), P()
    prefix_spec = P(None, home, None, None)
    cache_spec = P(None, home, None, None, None)

    def local_step(hidden, seq_lens, w_query, w_key, w_value, w_out, k_prefix, v_prefix, k_suffix, v_suffix):
        layers, dim, q_width = w_query.shape
        rows = hidden.shape[0]
        span, heads, hd = k_prefix.shape[1:]
        slots = k_suffix.shape[2]
        group = q_width // (heads * hd)
        chips = ctx_size // 2
        half, kc = dim // 2, dim // 4
        nblk = half // COLS
        qh = heads * group
        vmem, smem, anym = pltpu.VMEM, pltpu.SMEM, pl.ANY
        dma = pltpu.SemaphoreType.DMA
        spec = pl.BlockSpec
        scratch = [
            smem((rows,), jnp.int32), dma((3,)),
            vmem((RING, kc, (group + 2) * hd), BF16), dma((RING, 3)),
            vmem((chips, nblk, 2 * group * hd, COLS), BF16), dma((chips, nblk)),
            vmem((2, span, heads, hd), BF16), dma((2,)), vmem((64 * heads, hd), F32),
            vmem((layers, ctx_size, 2, span, hd), BF16), vmem((layers, 2, ctx_size, span, hd), BF16),
            dma((layers, 2, ctx_size)), dma((layers, 2, ctx_size)),
            vmem((2, rows, slots * heads, hd), BF16), dma((2,)),
            vmem((layers, 2, 2 * rows, half), BF16), vmem((2, rows, half), BF16), vmem((rows, half), BF16), dma((3, 2)),
            vmem((chips, 2 * rows, (group + 2) * hd), F32),
            vmem((layers, chips, 2, group + 2, rows, hd), BF16), vmem((layers, heads, group + 2, rows, hd), BF16),
            dma((layers, chips)), dma((layers, chips)),
            vmem((layers, chips, 2, group, rows, hd), BF16), dma((layers, chips)), dma((layers, chips)),
            vmem((rows * (qh + PAD), hd), F32), vmem((rows * (qh + PAD), hd), F32), vmem((rows * (qh + PAD), hd), F32),
            vmem((rows * qh, hd), F32),
            vmem((ctx_size, 2 * group * rows, span), F32), vmem((2 * group * rows, ctx_size * span), BF16),
            vmem((layers, chips, 2, group, rows, hd), BF16), vmem((layers, chips, 2, 8, 128), F32),
            vmem((layers, heads, group, rows, hd), BF16), vmem((layers, heads, 8, 128), F32),
            dma((layers, chips, 2)), dma((layers, heads)), dma((layers, chips, 2)), dma((layers, heads)),
            vmem((layers, 2, chips, rows, 2 * group * hd), BF16), dma((layers, chips)), dma((layers, chips)),
            vmem((nblk, 2 * rows, COLS), F32),
        ]
        hid, kvn = pl.pallas_call(
            functools.partial(decode_kernel, ctx_size),
            name="decode",
            out_shape=(jax.ShapeDtypeStruct((2, rows, half), BF16),
                       jax.ShapeDtypeStruct((layers, heads, 2, rows, hd), BF16)),
            in_specs=[spec(memory_space=anym)] * 10,
            out_specs=(spec(memory_space=anym), spec(memory_space=anym)),
            scratch_shapes=scratch,
            compiler_params=pltpu.CompilerParams(collective_id=0, has_side_effects=True, vmem_limit_bytes=67043328),
        )(hidden, seq_lens, w_query, w_key, w_value, w_out, k_prefix, v_prefix,
          k_suffix.reshape(layers, rows, slots * heads, hd), v_suffix.reshape(layers, rows, slots * heads, hd))
        copies = layers * 2 * (rows // 8)
        return pl.pallas_call(
            cache_kernel,
            name="caches",
            out_shape=(jax.ShapeDtypeStruct(hidden.shape, BF16), jax.ShapeDtypeStruct(k_suffix.shape, BF16),
                       jax.ShapeDtypeStruct(v_suffix.shape, BF16)),
            in_specs=[spec(memory_space=smem)] + [spec(memory_space=anym)] * 4,
            out_specs=(spec(memory_space=anym), spec(memory_space=anym), spec(memory_space=anym)),
            scratch_shapes=[vmem((layers, 2, rows, slots, heads, hd), BF16), vmem((layers, 2, rows * heads, hd), F32),
                            vmem((rows, dim), BF16), vmem((layers, heads, 2, rows, hd), BF16),
                            dma((copies,)), dma((copies,)), dma((4,))],
            compiler_params=pltpu.CompilerParams(vmem_limit_bytes=67043328),
        )(seq_lens, hid, kvn, k_suffix, v_suffix)

    return jax.shard_map(local_step, mesh=mesh,
                         in_specs=(row_spec, lens_spec, whole, whole, whole, whole, prefix_spec, prefix_spec, cache_spec, cache_spec),
                         out_specs=(row_spec, cache_spec, cache_spec), check_vma=False)
```

```python
import functools

import jax
import jax.numpy as jnp
from jax import lax
from jax.experimental import pallas as pl
from jax.experimental.pallas import tpu as pltpu
from jax.sharding import PartitionSpec as P

MESH = pl.DeviceIdType.MESH
BF16 = jnp.bfloat16
F32 = jnp.float32
RING = 10
COLS = 512
PAD = 8
LOG2E = 1.4426950408889634
FLOOR = float(jnp.finfo(jnp.float32).min)


def dot(a, b):
    return lax.dot_general(a, b, (((1,), (0,)), ((), ())), preferred_element_type=F32)


def dot_t(a, b):
    return lax.dot_general(a, b, (((1,), (1,)), ((), ())), preferred_element_type=F32)


def decode_kernel(ctx_size, hidden, lens_hbm, wq, wk, wv, wo, kpre, vpre, ksuf, vsuf, hid_out, kvn_out,
                  lens, io_sem, ring, w_sem, wo_buf, wo_sem, pst, pst_sem, pf32, psend, precv, ps_s, ps_r,
                  suf, suf_sem, xh, fin_st, fin_rc, x_sem, acc, qkv_st, hq, hs_s, hs_r,
                  q_rc, q_s, q_r, qs, os, ls, lm, sc, pb, o_st, lse_st, o_rc, lse_rc, o_s, o_r, l_s, l_r,
                  o_cat, oc_s, oc_r, acc_o):
    layers = wq.shape[0]
    dim = wq.shape[1]
    half = dim // 2
    kc = dim // 4
    rows, heads, hd = hidden.shape[0], kpre.shape[2], kpre.shape[3]
    qh = (wq.shape[2] // hd)
    group = wq.shape[2] // (heads * hd)
    span = kpre.shape[1]
    slots = ksuf.shape[2] // heads
    chips = ctx_size // 2
    order = (2, 1, 3, 0)
    scale = hd ** -0.5
    c2 = scale * LOG2E
    gq = group * hd
    nblk = half // COLS
    pitch = qh + PAD

    me = lax.axis_index("ctx")
    chip = me // 2
    core = me % 2
    other = 1 - core
    partner = chip * 2 + other
    pending = []

    def to(dev):
        return {"ctx": dev}

    def remote(src, dst, s_sem, r_sem, dev):
        return pltpu.make_async_remote_copy(src_ref=src, dst_ref=dst, send_sem=s_sem, recv_sem=r_sem,
                                            device_id=to(dev), device_id_type=MESH)

    def send(src, dst, s_sem, r_sem, dev):
        copy = remote(src, dst, s_sem, r_sem, dev)
        copy.start()
        pending.append(copy)

    def arrived(dst, r_sem, s_sem):
        remote(dst, dst, s_sem, r_sem, partner).wait_recv()

    def dest_chip(t):
        return (chip + order[t]) % chips

    def src_chip(t):
        return (chip + chips - order[t]) % chips

    def weight_place(layer, n):
        if layer == 0:
            return n // 4, (n // 2) % 2, n % 2
        return (n // 2) % chips, n // (2 * chips), n % 2

    def weight_copies(layer, n):
        t, hh, kk = weight_place(layer, n)
        slot = (layer * 4 * chips + n) % RING
        g = dest_chip(t) * 2 + core
        krows = pl.ds(pl.multiple_of(((core + hh) % 2) * half + kk * kc, 128), kc)
        qcols = pl.ds(pl.multiple_of(g * gq, gq), gq)
        kcols = pl.ds(pl.multiple_of(g * hd, hd), hd)
        return (
            pltpu.make_async_copy(wq.at[layer, krows, qcols], ring.at[slot, :, 0:gq], w_sem.at[slot, 0]),
            pltpu.make_async_copy(wk.at[layer, krows, kcols], ring.at[slot, :, gq:gq + hd], w_sem.at[slot, 1]),
            pltpu.make_async_copy(wv.at[layer, krows, kcols], ring.at[slot, :, gq + hd:gq + 2 * hd], w_sem.at[slot, 2]),
        )

    def fetch_weights(layer, first, last):
        for n in range(first, min(last, 4 * chips)):
            for copy in weight_copies(layer, n):
                copy.start()

    def wo_copy(layer, tc, nb):
        return pltpu.make_async_copy(
            wo.at[layer, pl.ds(pl.multiple_of(tc * 2 * gq, 2 * gq), 2 * gq),
                  pl.ds(pl.multiple_of(core * half + nb * COLS, COLS), COLS)],
            wo_buf.at[tc, nb], wo_sem.at[tc, nb])

    def fetch_wo(layer, tc):
        for nb in range(nblk):
            wo_copy(layer, tc, nb).start()

    def prefix_copies(layer):
        return (pltpu.make_async_copy(kpre.at[layer], pst.at[0], pst_sem.at[0]),
                pltpu.make_async_copy(vpre.at[layer], pst.at[1], pst_sem.at[1]))

    def suffix_copies(layer):
        return (pltpu.make_async_copy(ksuf.at[layer], suf.at[0], suf_sem.at[0]),
                pltpu.make_async_copy(vsuf.at[layer], suf.at[1], suf_sem.at[1]))

    def relayout_prefix(layer, kv):
        prefix_copies(layer)[kv].wait()
        step = 64

        @pl.loop(0, span // step)
        def _(blk):
            base = pl.multiple_of(blk * step, step)
            pf32[...] = pst[kv, pl.ds(base, step)].astype(F32).reshape(step * heads, hd)
            for g in range(heads):
                psend[layer, g, kv, pl.ds(base, step), :] = pf32[pl.ds(g, step, stride=heads), :].astype(BF16)

    def send_prefix(layer, kv, far, near):
        steps = ((2, core), (2, other), (0, other)) if far else ()
        steps += ((1, core), (3, core), (1, other), (3, other)) if near else ()
        for dc, cr in steps:
            dev = ((chip + dc) % chips) * 2 + cr
            send(psend.at[layer, dev, kv], precv.at[layer, kv, me], ps_s.at[layer, kv, dev], ps_r.at[layer, kv, me], dev)
        if near:
            precv[layer, kv, me] = psend[layer, me, kv]

    def await_prefix(layer):
        for d in (1, 7, 2, 6, 3, 5, 4):
            src = (me + d) % ctx_size
            for kv in range(2):
                arrived(precv.at[layer, kv, src], ps_r.at[layer, kv, src], ps_s.at[layer, kv, src])

    def dots(layer, chunks):
        for n in chunks:
            for copy in weight_copies(layer, n):
                copy.wait()
        total = None
        for n in chunks:
            _, hh, kk = weight_place(layer, n)
            slot = (layer * 4 * chips + n) % RING
            part = dot(xh[layer, (core + hh) % 2, :, kk * kc:(kk + 1) * kc], ring[slot])
            total = part if total is None else total + part
        return total

    def project(layer, t):
        if layer == 0:
            chunks = range(4 * t, 4 * t + 4)
            total = dots(layer, chunks)
        else:
            chunks = range(2 * chips + 2 * t, 2 * chips + 2 * t + 2)
            total = acc[t] + dots(layer, chunks)
        qkv = total.astype(BF16)
        for n in chunks:
            fetch_weights(layer, n + RING, n + RING + 1)
        if layer == 0 and t >= 2:
            fetch_wo(0, 2 * (t - 2))
            fetch_wo(0, 2 * (t - 2) + 1)

        for cr in range(2):
            part = slice(cr * rows, (cr + 1) * rows)
            for j in range(group):
                qkv_st[layer, t, cr, j] = qkv[part, j * hd:(j + 1) * hd]
            for i in range(2):
                qkv_st[layer, t, cr, group + i] = qkv[part, gq + i * hd:gq + (i + 1) * hd]
        tc = dest_chip(t)
        if order[t] != 0:
            send(qkv_st.at[layer, t, :, 0:group], q_rc.at[layer, chip], q_s.at[layer, t], q_r.at[layer, chip],
                 tc * 2 + core)
        else:
            q_rc[layer, chip] = qkv_st[layer, t, :, 0:group]
        g = tc * 2 + core
        send(qkv_st.at[layer, t, other], hq.at[layer, g], hs_s.at[layer, t], hs_r.at[layer, t], partner)
        hq[layer, g] = qkv_st[layer, t, core]

    def suffix_queries(layer):
        for t in range(chips):
            arrived(hq.at[layer, dest_chip(t) * 2 + other], hs_r.at[layer, t], hs_s.at[layer, t])
        for g in range(heads):
            for j in range(group):
                qs[pl.ds(g * group + j, rows, stride=pitch), :] = hq[layer, g, j].astype(F32)
        for copy in suffix_copies(layer):
            copy.wait()

    def suffix_attention(layer, first, last):
        row_id = lax.broadcasted_iota(jnp.int32, (qh, slots * heads), 0)
        col_id = lax.broadcasted_iota(jnp.int32, (qh, slots * heads), 1)
        slot_of = jnp.where((row_id // group) == (col_id % heads), col_id // heads, slots)
        step = 8

        @pl.loop(first // step, last // step)
        def _(blk):
            for i in range(step):
                b = blk * step + i
                base = pl.multiple_of(b * pitch, 8)
                s = dot_t(qs[pl.ds(base, qh), :].astype(BF16), suf[0, b])
                s = jnp.where(slot_of < lens[b], s, FLOOR)
                m = jnp.max(s, axis=1, keepdims=True)
                e = jnp.exp2((s - m) * c2)
                mass = jnp.sum(e, axis=1, keepdims=True)
                val = dot(e.astype(BF16), suf[1, b])
                os[pl.ds(base, qh), :] = val * (1.0 / mass)
                ls[pl.ds(base, qh), :] = jnp.broadcast_to(m * scale + jnp.log(mass), (qh, hd))

    def suffix_merge(layer):
        for g in range(heads):
            k_new = hq[layer, g, group].astype(F32)
            v_new = hq[layer, g, group + 1].astype(F32)
            for j in range(group):
                h = g * group + j
                picked = pl.ds(h, rows, stride=pitch)
                lo = ls[picked, :]
                sn = jnp.sum(hq[layer, g, j].astype(F32) * k_new, axis=1, keepdims=True) * scale
                top = jnp.maximum(lo, sn)
                w_old = jnp.exp(lo - top)
                w_new = jnp.exp(sn - top)
                mass = w_old + w_new
                qs[h * rows:(h + 1) * rows, :] = (w_old * os[picked, :] + w_new * v_new) / mass
                lm[h * rows:(h + 1) * rows, :] = top + jnp.log(mass)

    def prefix_attention(layer, t):
        src = src_chip(t)
        if order[t] != 0:
            arrived(q_rc.at[layer, src], q_r.at[layer, src], q_s.at[layer, t])
        q = q_rc[layer, src].reshape(2 * group * rows, hd)
        peak = None
        for s in range(ctx_size):
            part = dot_t(q, precv[layer, 0, s])
            sc[s] = part
            for lo in range(0, span, 128):
                piece = part[:, lo:lo + 128]
                peak = piece if peak is None else jnp.maximum(peak, piece)
        m = jnp.max(peak, axis=1, keepdims=True)
        mass = jnp.zeros((2 * group * rows, 128), F32)
        for s in range(ctx_size):
            e = jnp.exp2((sc[s] - m) * c2)
            for lo in range(0, span, 128):
                mass = mass + e[:, lo:lo + 128]
            pb[:, s * span:(s + 1) * span] = e.astype(BF16)
        mass = jnp.sum(mass, axis=1, keepdims=True)
        vals = dot(pb[...], precv[layer, 1].reshape(ctx_size * span, hd))
        out = (vals * (1.0 / mass)).astype(BF16)
        lse = jnp.broadcast_to(m * scale + jnp.log(mass), (2 * group * rows, 128)).T
        for cr in range(2):
            part = group * rows
            o_st[layer, t, cr] = out[cr * part:(cr + 1) * part].reshape(group, rows, hd)
            lse_st[layer, t, cr] = lse[0:8, cr * part:(cr + 1) * part]
        if order[t] != 0:
            for cr in range(2):
                dev = src * 2 + cr
                send(lse_st.at[layer, t, cr], lse_rc.at[layer, me], l_s.at[layer, t, cr], l_r.at[layer, me], dev)
                send(o_st.at[layer, t, cr], o_rc.at[layer, me], o_s.at[layer, t, cr], o_r.at[layer, me], dev)
        else:
            send(lse_st.at[layer, t, other], lse_rc.at[layer, me], l_s.at[layer, t, 0], l_r.at[layer, me], partner)
            send(o_st.at[layer, t, other], o_rc.at[layer, me], o_s.at[layer, t, 0], o_r.at[layer, me], partner)
            lse_rc[layer, me] = lse_st[layer, t, core]
            o_rc[layer, me] = o_st[layer, t, core]

    def combine(layer, t):
        tc = dest_chip(t)
        for par in range(2):
            if order[t] != 0:
                g = tc * 2 + par
                arrived(lse_rc.at[layer, g], l_r.at[layer, g], l_s.at[layer, t, 0])
                arrived(o_rc.at[layer, g], o_r.at[layer, g], o_s.at[layer, t, 0])
            elif par == 0:
                arrived(lse_rc.at[layer, partner], l_r.at[layer, partner], l_s.at[layer, t, 0])
                arrived(o_rc.at[layer, partner], o_r.at[layer, partner], o_s.at[layer, t, 0])
        for par in range(2):
            g = tc * 2 + par
            lse_p = jnp.broadcast_to(lse_rc[layer, g, 0:1, :], (group * rows, 128)).T
            for j in range(group):
                here = pl.ds(pl.multiple_of((g * group + j) * rows, rows), rows)
                lp = lse_p[j * rows:(j + 1) * rows]
                lo = lm[here, :]
                top = jnp.maximum(lp, lo)
                wp = jnp.exp(lp - top)
                ws = jnp.exp(lo - top)
                mixed = wp * o_rc[layer, g, j].astype(F32) + ws * qs[here, :]
                at = (par * group + j) * hd
                o_cat[layer, core, tc, :, at:at + hd] = (mixed / (wp + ws)).astype(BF16)
        send(o_cat.at[layer, core, tc], o_cat.at[layer, core, tc], oc_s.at[layer, t], oc_r.at[layer, t], partner)

    def project_out(layer, t):
        tc = dest_chip(t)
        arrived(o_cat.at[layer, other, tc], oc_r.at[layer, t], oc_s.at[layer, t])
        lhs = jnp.concatenate([o_cat[layer, 0, tc], o_cat[layer, 1, tc]], axis=0)

        for nb in range(nblk):
            wo_copy(layer, tc, nb).wait()
        for nb in range(nblk):
            upd = dot(lhs, wo_buf[tc, nb])
            if t == 0:
                acc_o[nb] = upd
            else:
                acc_o[nb] += upd
            if layer + 1 < layers:
                wo_copy(layer + 1, tc, nb).start()

    own = pl.ds(pl.multiple_of(core * rows, rows), rows)
    theirs = pl.ds(pl.multiple_of(other * rows, rows), rows)
    barrier = pltpu.get_barrier_semaphore()
    for d in range(1, ctx_size):
        pl.semaphore_signal(barrier, inc=1, device_id=to((me + d) % ctx_size), device_id_type=MESH)
    for copy in prefix_copies(0):
        copy.start()
    loads = [pltpu.make_async_copy(lens_hbm, lens, io_sem.at[0])]
    for sd in range(2):
        loads.append(pltpu.make_async_copy(hidden.at[:, sd * half:(sd + 1) * half], xh.at[0, sd, own, :], io_sem.at[1 + sd]))
    for copy in loads:
        copy.start()
    for copy in loads:
        copy.wait()
    fetch_weights(0, 0, 2)
    relayout_prefix(0, 0)
    pl.semaphore_wait(barrier, ctx_size - 1)
    send(xh.at[0, :, own, :], xh.at[0, :, own, :], x_sem.at[2, 0], x_sem.at[2, 1], partner)
    send_prefix(0, 0, True, True)
    relayout_prefix(0, 1)
    send_prefix(0, 1, True, True)
    fetch_weights(0, 2, RING)
    arrived(xh.at[0, :, theirs, :], x_sem.at[2, 1], x_sem.at[2, 0])

    for layer in range(layers):
        if layer > 0:
            for t in range(chips):
                acc[t] = dots(layer, (2 * t, 2 * t + 1))
                for n in (2 * t, 2 * t + 1):
                    fetch_weights(layer, n + RING, n + RING + 1)
            arrived(xh.at[layer, other], x_sem.at[0, 1], x_sem.at[0, 0])
        for t in range(chips):
            project(layer, t)
            if layer == 0 and t == 1:
                for copy in suffix_copies(0) + prefix_copies(1):
                    copy.start()
        if layer + 1 < layers:
            fetch_weights(layer + 1, 0, RING)
            relayout_prefix(layer + 1, 0)
            send_prefix(layer + 1, 0, True, False)
            suffix_queries(layer)
            suffix_attention(layer, 0, rows)
            suffix_merge(layer)
            for copy in suffix_copies(layer + 1):
                copy.start()
            relayout_prefix(layer + 1, 1)
            await_prefix(layer)
            for t in range(chips):
                prefix_attention(layer, t)
            send_prefix(layer + 1, 0, False, True)
            send_prefix(layer + 1, 1, True, True)
        else:
            await_prefix(layer)
            prefix_attention(layer, chips - 1)
            suffix_queries(layer)
            suffix_attention(layer, 0, rows // 2)
            for t in range(chips - 1):
                prefix_attention(layer, t)
            suffix_attention(layer, rows // 2, rows)
            suffix_merge(layer)
        for t in range(chips):
            combine(layer, t)
            if t > 0:
                project_out(layer, t - 1)
        project_out(layer, chips - 1)
        for nb in range(nblk):
            cols = slice(nb * COLS, (nb + 1) * COLS)
            new = (xh[layer, core, :, cols].astype(F32) + acc_o[nb].astype(BF16).astype(F32)).astype(BF16)
            if layer + 1 < layers:
                xh[layer + 1, core, :, cols] = new
            else:
                for cr in range(2):
                    fin_st[cr, :, cols] = new[cr * rows:(cr + 1) * rows]
        if layer + 1 < layers:
            send(xh.at[layer + 1, core], xh.at[layer + 1, core], x_sem.at[0, 0], x_sem.at[0, 1], partner)
    send(fin_st.at[other], fin_rc, x_sem.at[1, 0], x_sem.at[1, 1], partner)
    stores = [pltpu.make_async_copy(fin_st.at[core], hid_out.at[core], io_sem.at[0]),
              pltpu.make_async_copy(hq.at[:, :, group:group + 2], kvn_out, io_sem.at[1])]
    for copy in stores:
        copy.start()
    arrived(fin_rc, x_sem.at[1, 1], x_sem.at[1, 0])
    stores.append(pltpu.make_async_copy(fin_rc, hid_out.at[other], io_sem.at[2]))
    stores[2].start()
    for copy in stores:
        copy.wait()
    for copy in pending:
        copy.wait_send()


def cache_kernel(lens_hbm, hid, kvn, ksuf, vsuf, hid_out, kout, vout, lens, buf, tiles, hbuf, kvbuf, in_sem, out_sem, io_sem):
    layers, batch = ksuf.shape[0], ksuf.shape[1]
    heads = ksuf.shape[3]
    half = hid.shape[2]
    step = 8
    parts = batch // step
    srcs, dsts = (ksuf, vsuf), (kout, vout)

    def copies(layer, i, part, out):
        here = pl.ds(part * step, step)
        at = (layer * 2 + i) * parts + part
        if out:
            return pltpu.make_async_copy(buf.at[layer, i, here], dsts[i].at[layer, here], out_sem.at[at])
        return pltpu.make_async_copy(srcs[i].at[layer, here], buf.at[layer, i, here], in_sem.at[at])

    todo = [(layer, i, part) for layer in range(layers) for i in range(2) for part in range(parts)]
    news = pltpu.make_async_copy(kvn, kvbuf, io_sem.at[0])
    news.start()
    lengths = pltpu.make_async_copy(lens_hbm, lens, io_sem.at[4])
    lengths.start()
    for layer, i, part in todo:
        copies(layer, i, part, False).start()
    sides = [pltpu.make_async_copy(hid.at[sd], hbuf.at[:, sd * half:(sd + 1) * half], io_sem.at[1 + sd]) for sd in range(2)]
    for copy in sides:
        copy.start()
    news.wait()
    lengths.wait()
    for layer in range(layers):
        for i in range(2):
            for g in range(heads):
                tiles[layer, i, pl.ds(g, batch, stride=heads), :] = kvbuf[layer, g, i].astype(F32)
    for layer, i, part in todo:
        copies(layer, i, part, False).wait()
        for b in range(part * step, (part + 1) * step):
            buf[layer, i, b, lens[b]] = tiles[layer, i, b * heads:(b + 1) * heads, :].astype(BF16)
        copies(layer, i, part, True).start()
    for copy in sides:
        copy.wait()
    whole = pltpu.make_async_copy(hbuf, hid_out, io_sem.at[3])
    whole.start()
    for layer, i, part in todo:
        copies(layer, i, part, True).wait()
    whole.wait()


def solution(mesh):
    ctx_size = mesh.shape["ctx"]
    home = ("data", "ctx")
    row_spec, lens_spec, whole = P(home, None), P(home), P()
    prefix_spec = P(None, home, None, None)
    cache_spec = P(None, home, None, None, None)

    def local_step(hidden, seq_lens, w_query, w_key, w_value, w_out, k_prefix, v_prefix, k_suffix, v_suffix):
        layers, dim, q_width = w_query.shape
        rows = hidden.shape[0]
        span, heads, hd = k_prefix.shape[1:]
        slots = k_suffix.shape[2]
        group = q_width // (heads * hd)
        chips = ctx_size // 2
        half, kc = dim // 2, dim // 4
        nblk = half // COLS
        qh = heads * group
        vmem, smem, anym = pltpu.VMEM, pltpu.SMEM, pl.ANY
        dma = pltpu.SemaphoreType.DMA
        spec = pl.BlockSpec
        scratch = [
            smem((rows,), jnp.int32), dma((3,)),
            vmem((RING, kc, (group + 2) * hd), BF16), dma((RING, 3)),
            vmem((chips, nblk, 2 * group * hd, COLS), BF16), dma((chips, nblk)),
            vmem((2, span, heads, hd), BF16), dma((2,)), vmem((64 * heads, hd), F32),
            vmem((layers, ctx_size, 2, span, hd), BF16), vmem((layers, 2, ctx_size, span, hd), BF16),
            dma((layers, 2, ctx_size)), dma((layers, 2, ctx_size)),
            vmem((2, rows, slots * heads, hd), BF16), dma((2,)),
            vmem((layers, 2, 2 * rows, half), BF16), vmem((2, rows, half), BF16), vmem((rows, half), BF16), dma((3, 2)),
            vmem((chips, 2 * rows, (group + 2) * hd), F32),
            vmem((layers, chips, 2, group + 2, rows, hd), BF16), vmem((layers, heads, group + 2, rows, hd), BF16),
            dma((layers, chips)), dma((layers, chips)),
            vmem((layers, chips, 2, group, rows, hd), BF16), dma((layers, chips)), dma((layers, chips)),
            vmem((rows * (qh + PAD), hd), F32), vmem((rows * (qh + PAD), hd), F32), vmem((rows * (qh + PAD), hd), F32),
            vmem((rows * qh, hd), F32),
            vmem((ctx_size, 2 * group * rows, span), F32), vmem((2 * group * rows, ctx_size * span), BF16),
            vmem((layers, chips, 2, group, rows, hd), BF16), vmem((layers, chips, 2, 8, 128), F32),
            vmem((layers, heads, group, rows, hd), BF16), vmem((layers, heads, 8, 128), F32),
            dma((layers, chips, 2)), dma((layers, heads)), dma((layers, chips, 2)), dma((layers, heads)),
            vmem((layers, 2, chips, rows, 2 * group * hd), BF16), dma((layers, chips)), dma((layers, chips)),
            vmem((nblk, 2 * rows, COLS), F32),
        ]
        hid, kvn = pl.pallas_call(
            functools.partial(decode_kernel, ctx_size),
            name="decode",
            out_shape=(jax.ShapeDtypeStruct((2, rows, half), BF16),
                       jax.ShapeDtypeStruct((layers, heads, 2, rows, hd), BF16)),
            in_specs=[spec(memory_space=anym)] * 10,
            out_specs=(spec(memory_space=anym), spec(memory_space=anym)),
            scratch_shapes=scratch,
            compiler_params=pltpu.CompilerParams(collective_id=0, has_side_effects=True, vmem_limit_bytes=67043328),
        )(hidden, seq_lens, w_query, w_key, w_value, w_out, k_prefix, v_prefix,
          k_suffix.reshape(layers, rows, slots * heads, hd), v_suffix.reshape(layers, rows, slots * heads, hd))
        copies = layers * 2 * (rows // 8)
        return pl.pallas_call(
            cache_kernel,
            name="caches",
            out_shape=(jax.ShapeDtypeStruct(hidden.shape, BF16), jax.ShapeDtypeStruct(k_suffix.shape, BF16),
                       jax.ShapeDtypeStruct(v_suffix.shape, BF16)),
            in_specs=[spec(memory_space=anym)] * 5,
            out_specs=(spec(memory_space=anym), spec(memory_space=anym), spec(memory_space=anym)),
            scratch_shapes=[smem((rows,), jnp.int32), vmem((layers, 2, rows, slots, heads, hd), BF16),
                            vmem((layers, 2, rows * heads, hd), F32),
                            vmem((rows, dim), BF16), vmem((layers, heads, 2, rows, hd), BF16),
                            dma((copies,)), dma((copies,)), dma((5,))],
            compiler_params=pltpu.CompilerParams(vmem_limit_bytes=67043328),
        )(seq_lens, hid, kvn, k_suffix, v_suffix)

    return jax.shard_map(local_step, mesh=mesh,
                         in_specs=(row_spec, lens_spec, whole, whole, whole, whole, prefix_spec, prefix_spec, cache_spec, cache_spec),
                         out_specs=(row_spec, cache_spec, cache_spec), check_vma=False)
```

```python
import functools

import jax
import jax.numpy as jnp
from jax import lax
from jax.experimental import pallas as pl
from jax.experimental.pallas import tpu as pltpu
from jax.sharding import PartitionSpec as P

MESH = pl.DeviceIdType.MESH
BF16 = jnp.bfloat16
F32 = jnp.float32
RING = 10
COLS = 512
PAD = 8
LOG2E = 1.4426950408889634
FLOOR = float(jnp.finfo(jnp.float32).min)


def dot(a, b):
    return lax.dot_general(a, b, (((1,), (0,)), ((), ())), preferred_element_type=F32)


def dot_t(a, b):
    return lax.dot_general(a, b, (((1,), (1,)), ((), ())), preferred_element_type=F32)


def decode_kernel(ctx_size, hidden, lens_hbm, wq, wk, wv, wo, kpre, vpre, ksuf, vsuf, hid_out, kvn_out,
                  lens, io_sem, ring, w_sem, wo_buf, wo_sem, pst, pst_sem, pf32, psend, precv, ps_s, ps_r,
                  suf, suf_sem, xh, fin_st, fin_rc, x_sem, acc, qkv_st, hq, hs_s, hs_r,
                  q_rc, q_s, q_r, qs, os, ls, lm, sc, pb, o_st, lse_st, o_rc, lse_rc, o_s, o_r, l_s, l_r,
                  o_cat, oc_s, oc_r, acc_o):
    layers = wq.shape[0]
    dim = wq.shape[1]
    half = dim // 2
    kc = dim // 4
    rows, heads, hd = hidden.shape[0], kpre.shape[2], kpre.shape[3]
    qh = (wq.shape[2] // hd)
    group = wq.shape[2] // (heads * hd)
    span = kpre.shape[1]
    slots = ksuf.shape[2] // heads
    chips = ctx_size // 2
    order = (2, 1, 3, 0)
    scale = hd ** -0.5
    c2 = scale * LOG2E
    gq = group * hd
    nblk = half // COLS
    pitch = qh + PAD

    me = lax.axis_index("ctx")
    chip = me // 2
    core = me % 2
    other = 1 - core
    partner = chip * 2 + other
    pending = []

    def to(dev):
        return {"ctx": dev}

    def remote(src, dst, s_sem, r_sem, dev):
        return pltpu.make_async_remote_copy(src_ref=src, dst_ref=dst, send_sem=s_sem, recv_sem=r_sem,
                                            device_id=to(dev), device_id_type=MESH)

    def send(src, dst, s_sem, r_sem, dev):
        copy = remote(src, dst, s_sem, r_sem, dev)
        copy.start()
        pending.append(copy)

    def arrived(dst, r_sem, s_sem):
        remote(dst, dst, s_sem, r_sem, partner).wait_recv()

    def dest_chip(t):
        return (chip + order[t]) % chips

    def src_chip(t):
        return (chip + chips - order[t]) % chips

    def weight_place(layer, n):
        if layer == 0:
            return n // 4, (n // 2) % 2, n % 2
        return (n // 2) % chips, n // (2 * chips), n % 2

    def weight_copies(layer, n):
        t, hh, kk = weight_place(layer, n)
        slot = (layer * 4 * chips + n) % RING
        g = dest_chip(t) * 2 + core
        krows = pl.ds(pl.multiple_of(((core + hh) % 2) * half + kk * kc, 128), kc)
        qcols = pl.ds(pl.multiple_of(g * gq, gq), gq)
        kcols = pl.ds(pl.multiple_of(g * hd, hd), hd)
        return (
            pltpu.make_async_copy(wq.at[layer, krows, qcols], ring.at[slot, :, 0:gq], w_sem.at[slot, 0]),
            pltpu.make_async_copy(wk.at[layer, krows, kcols], ring.at[slot, :, gq:gq + hd], w_sem.at[slot, 1]),
            pltpu.make_async_copy(wv.at[layer, krows, kcols], ring.at[slot, :, gq + hd:gq + 2 * hd], w_sem.at[slot, 2]),
        )

    def fetch_weights(layer, first, last):
        for n in range(first, min(last, 4 * chips)):
            for copy in weight_copies(layer, n):
                copy.start()

    def wo_copy(layer, tc, nb):
        return pltpu.make_async_copy(
            wo.at[layer, pl.ds(pl.multiple_of(tc * 2 * gq, 2 * gq), 2 * gq),
                  pl.ds(pl.multiple_of(core * half + nb * COLS, COLS), COLS)],
            wo_buf.at[tc, nb], wo_sem.at[tc, nb])

    def fetch_wo(layer, tc):
        for nb in range(nblk):
            wo_copy(layer, tc, nb).start()

    def prefix_copies(layer):
        return (pltpu.make_async_copy(kpre.at[layer], pst.at[0], pst_sem.at[0]),
                pltpu.make_async_copy(vpre.at[layer], pst.at[1], pst_sem.at[1]))

    def suffix_copies(layer):
        return (pltpu.make_async_copy(ksuf.at[layer], suf.at[0], suf_sem.at[0]),
                pltpu.make_async_copy(vsuf.at[layer], suf.at[1], suf_sem.at[1]))

    def relayout_prefix(layer, kv):
        prefix_copies(layer)[kv].wait()
        step = 64

        @pl.loop(0, span // step)
        def _(blk):
            base = pl.multiple_of(blk * step, step)
            pf32[...] = pst[kv, pl.ds(base, step)].astype(F32).reshape(step * heads, hd)
            for g in range(heads):
                psend[layer, g, kv, pl.ds(base, step), :] = pf32[pl.ds(g, step, stride=heads), :].astype(BF16)

    def send_prefix(layer, kv, far, near):
        steps = ((2, core), (2, other), (0, other)) if far else ()
        steps += ((1, core), (3, core), (1, other), (3, other)) if near else ()
        for dc, cr in steps:
            dev = ((chip + dc) % chips) * 2 + cr
            send(psend.at[layer, dev, kv], precv.at[layer, kv, me], ps_s.at[layer, kv, dev], ps_r.at[layer, kv, me], dev)
        if near:
            precv[layer, kv, me] = psend[layer, me, kv]

    def await_prefix(layer, kv):
        for d in (1, 7, 2, 6, 3, 5, 4):
            src = (me + d) % ctx_size
            arrived(precv.at[layer, kv, src], ps_r.at[layer, kv, src], ps_s.at[layer, kv, src])

    def dots(layer, chunks):
        for n in chunks:
            for copy in weight_copies(layer, n):
                copy.wait()
        total = None
        for n in chunks:
            _, hh, kk = weight_place(layer, n)
            slot = (layer * 4 * chips + n) % RING
            part = dot(xh[layer, (core + hh) % 2, :, kk * kc:(kk + 1) * kc], ring[slot])
            total = part if total is None else total + part
        return total

    def project(layer, t):
        if layer == 0:
            chunks = range(4 * t, 4 * t + 4)
            total = dots(layer, chunks)
        else:
            chunks = range(2 * chips + 2 * t, 2 * chips + 2 * t + 2)
            total = acc[t] + dots(layer, chunks)
        qkv = total.astype(BF16)
        for n in chunks:
            fetch_weights(layer, n + RING, n + RING + 1)
        if t >= 2:
            fetch_wo(layer, 2 * (t - 2))
            fetch_wo(layer, 2 * (t - 2) + 1)

        for cr in range(2):
            part = slice(cr * rows, (cr + 1) * rows)
            for j in range(group):
                qkv_st[layer, t, cr, j] = qkv[part, j * hd:(j + 1) * hd]
            for i in range(2):
                qkv_st[layer, t, cr, group + i] = qkv[part, gq + i * hd:gq + (i + 1) * hd]
        tc = dest_chip(t)
        if order[t] != 0:
            send(qkv_st.at[layer, t, :, 0:group], q_rc.at[layer, chip], q_s.at[layer, t], q_r.at[layer, chip],
                 tc * 2 + core)
        else:
            q_rc[layer, chip] = qkv_st[layer, t, :, 0:group]
        g = tc * 2 + core
        send(qkv_st.at[layer, t, other], hq.at[layer, g], hs_s.at[layer, t], hs_r.at[layer, t], partner)
        hq[layer, g] = qkv_st[layer, t, core]

    def suffix_queries(layer):
        for t in range(chips):
            arrived(hq.at[layer, dest_chip(t) * 2 + other], hs_r.at[layer, t], hs_s.at[layer, t])
        for g in range(heads):
            for j in range(group):
                qs[pl.ds(g * group + j, rows, stride=pitch), :] = hq[layer, g, j].astype(F32)
        for copy in suffix_copies(layer):
            copy.wait()

    def suffix_attention(layer, first, last):
        row_id = lax.broadcasted_iota(jnp.int32, (qh, slots * heads), 0)
        col_id = lax.broadcasted_iota(jnp.int32, (qh, slots * heads), 1)
        slot_of = jnp.where((row_id // group) == (col_id % heads), col_id // heads, slots)
        step = 8

        @pl.loop(first // step, last // step)
        def _(blk):
            for i in range(step):
                b = blk * step + i
                base = pl.multiple_of(b * pitch, 8)
                s = dot_t(qs[pl.ds(base, qh), :].astype(BF16), suf[0, b])
                s = jnp.where(slot_of < lens[b], s, FLOOR)
                m = jnp.max(s, axis=1, keepdims=True)
                e = jnp.exp2((s - m) * c2)
                mass = jnp.sum(e, axis=1, keepdims=True)
                val = dot(e.astype(BF16), suf[1, b])
                os[pl.ds(base, qh), :] = val * (1.0 / mass)
                ls[pl.ds(base, qh), :] = jnp.broadcast_to(m * scale + jnp.log(mass), (qh, hd))

    def suffix_merge(layer):
        for g in range(heads):
            k_new = hq[layer, g, group].astype(F32)
            v_new = hq[layer, g, group + 1].astype(F32)
            for j in range(group):
                h = g * group + j
                picked = pl.ds(h, rows, stride=pitch)
                lo = ls[picked, :]
                sn = jnp.sum(hq[layer, g, j].astype(F32) * k_new, axis=1, keepdims=True) * scale
                top = jnp.maximum(lo, sn)
                w_old = jnp.exp(lo - top)
                w_new = jnp.exp(sn - top)
                mass = w_old + w_new
                qs[h * rows:(h + 1) * rows, :] = (w_old * os[picked, :] + w_new * v_new) / mass
                lm[h * rows:(h + 1) * rows, :] = top + jnp.log(mass)

    def prefix_attention(layer, t):
        src = src_chip(t)
        if order[t] != 0:
            arrived(q_rc.at[layer, src], q_r.at[layer, src], q_s.at[layer, t])
        q = q_rc[layer, src].reshape(2 * group * rows, hd)
        peak = None
        for s in range(ctx_size):
            part = dot_t(q, precv[layer, 0, s])
            sc[s] = part
            for lo in range(0, span, 128):
                piece = part[:, lo:lo + 128]
                peak = piece if peak is None else jnp.maximum(peak, piece)
        m = jnp.max(peak, axis=1, keepdims=True)
        mass = jnp.zeros((2 * group * rows, 128), F32)
        for s in range(ctx_size):
            e = jnp.exp2((sc[s] - m) * c2)
            for lo in range(0, span, 128):
                mass = mass + e[:, lo:lo + 128]
            pb[:, s * span:(s + 1) * span] = e.astype(BF16)
        mass = jnp.sum(mass, axis=1, keepdims=True)
        if t == (0 if layer == 0 else chips - 1):
            await_prefix(layer, 1)
        vals = dot(pb[...], precv[layer, 1].reshape(ctx_size * span, hd))
        out = (vals * (1.0 / mass)).astype(BF16)
        lse = jnp.broadcast_to(m * scale + jnp.log(mass), (2 * group * rows, 128)).T
        for cr in range(2):
            part = group * rows
            o_st[layer, t, cr] = out[cr * part:(cr + 1) * part].reshape(group, rows, hd)
            lse_st[layer, t, cr] = lse[0:8, cr * part:(cr + 1) * part]
        if order[t] != 0:
            for cr in range(2):
                dev = src * 2 + cr
                send(lse_st.at[layer, t, cr], lse_rc.at[layer, me], l_s.at[layer, t, cr], l_r.at[layer, me], dev)
                send(o_st.at[layer, t, cr], o_rc.at[layer, me], o_s.at[layer, t, cr], o_r.at[layer, me], dev)
        else:
            send(lse_st.at[layer, t, other], lse_rc.at[layer, me], l_s.at[layer, t, 0], l_r.at[layer, me], partner)
            send(o_st.at[layer, t, other], o_rc.at[layer, me], o_s.at[layer, t, 0], o_r.at[layer, me], partner)
            lse_rc[layer, me] = lse_st[layer, t, core]
            o_rc[layer, me] = o_st[layer, t, core]

    def combine(layer, t):
        tc = dest_chip(t)
        for par in range(2):
            if order[t] != 0:
                g = tc * 2 + par
                arrived(lse_rc.at[layer, g], l_r.at[layer, g], l_s.at[layer, t, 0])
                arrived(o_rc.at[layer, g], o_r.at[layer, g], o_s.at[layer, t, 0])
            elif par == 0:
                arrived(lse_rc.at[layer, partner], l_r.at[layer, partner], l_s.at[layer, t, 0])
                arrived(o_rc.at[layer, partner], o_r.at[layer, partner], o_s.at[layer, t, 0])
        for par in range(2):
            g = tc * 2 + par
            lse_p = jnp.broadcast_to(lse_rc[layer, g, 0:1, :], (group * rows, 128)).T
            for j in range(group):
                here = pl.ds(pl.multiple_of((g * group + j) * rows, rows), rows)
                lp = lse_p[j * rows:(j + 1) * rows]
                lo = lm[here, :]
                top = jnp.maximum(lp, lo)
                wp = jnp.exp(lp - top)
                ws = jnp.exp(lo - top)
                mixed = wp * o_rc[layer, g, j].astype(F32) + ws * qs[here, :]
                at = (par * group + j) * hd
                o_cat[layer, core, tc, :, at:at + hd] = (mixed / (wp + ws)).astype(BF16)
        send(o_cat.at[layer, core, tc], o_cat.at[layer, core, tc], oc_s.at[layer, t], oc_r.at[layer, t], partner)

    def project_out(layer, t):
        tc = dest_chip(t)
        arrived(o_cat.at[layer, other, tc], oc_r.at[layer, t], oc_s.at[layer, t])
        lhs = jnp.concatenate([o_cat[layer, 0, tc], o_cat[layer, 1, tc]], axis=0)

        for nb in range(nblk):
            wo_copy(layer, tc, nb).wait()
        for nb in range(nblk):
            upd = dot(lhs, wo_buf[tc, nb])
            if t == 0:
                acc_o[nb] = upd
            else:
                acc_o[nb] += upd

    own = pl.ds(pl.multiple_of(core * rows, rows), rows)
    theirs = pl.ds(pl.multiple_of(other * rows, rows), rows)
    barrier = pltpu.get_barrier_semaphore()
    for d in range(1, ctx_size):
        pl.semaphore_signal(barrier, inc=1, device_id=to((me + d) % ctx_size), device_id_type=MESH)
    for copy in prefix_copies(0):
        copy.start()
    loads = [pltpu.make_async_copy(lens_hbm, lens, io_sem.at[0])]
    for sd in range(2):
        loads.append(pltpu.make_async_copy(hidden.at[:, sd * half:(sd + 1) * half], xh.at[0, sd, own, :], io_sem.at[1 + sd]))
    for copy in loads:
        copy.start()
    for copy in loads:
        copy.wait()
    fetch_weights(0, 0, 2)
    relayout_prefix(0, 0)
    pl.semaphore_wait(barrier, ctx_size - 1)
    send(xh.at[0, :, own, :], xh.at[0, :, own, :], x_sem.at[2, 0], x_sem.at[2, 1], partner)
    send_prefix(0, 0, True, True)
    relayout_prefix(0, 1)
    send_prefix(0, 1, True, True)
    fetch_weights(0, 2, RING)
    arrived(xh.at[0, :, theirs, :], x_sem.at[2, 1], x_sem.at[2, 0])

    for layer in range(layers):
        if layer > 0:
            for t in range(chips):
                acc[t] = dots(layer, (2 * t, 2 * t + 1))
                for n in (2 * t, 2 * t + 1):
                    fetch_weights(layer, n + RING, n + RING + 1)
            arrived(xh.at[layer, other], x_sem.at[0, 1], x_sem.at[0, 0])
        for t in range(chips):
            project(layer, t)
            if layer == 0 and t == 1:
                for copy in suffix_copies(0) + prefix_copies(1):
                    copy.start()
        if layer + 1 < layers:
            fetch_weights(layer + 1, 0, RING)
            relayout_prefix(layer + 1, 0)
            send_prefix(layer + 1, 0, True, False)
            suffix_queries(layer)
            suffix_attention(layer, 0, rows)
            suffix_merge(layer)
            for copy in suffix_copies(layer + 1):
                copy.start()
            relayout_prefix(layer + 1, 1)
            await_prefix(layer, 0)
            for t in range(chips):
                prefix_attention(layer, t)
            send_prefix(layer + 1, 0, False, True)
            send_prefix(layer + 1, 1, True, True)
        else:
            await_prefix(layer, 0)
            prefix_attention(layer, chips - 1)
            suffix_queries(layer)
            suffix_attention(layer, 0, rows // 2)
            for t in range(chips - 1):
                prefix_attention(layer, t)
            suffix_attention(layer, rows // 2, rows)
            suffix_merge(layer)
        for t in range(chips):
            combine(layer, t)
            if t > 0:
                project_out(layer, t - 1)
        project_out(layer, chips - 1)
        for nb in range(nblk):
            cols = slice(nb * COLS, (nb + 1) * COLS)
            new = (xh[layer, core, :, cols].astype(F32) + acc_o[nb].astype(BF16).astype(F32)).astype(BF16)
            if layer + 1 < layers:
                xh[layer + 1, core, :, cols] = new
            else:
                for cr in range(2):
                    fin_st[cr, :, cols] = new[cr * rows:(cr + 1) * rows]
        if layer + 1 < layers:
            send(xh.at[layer + 1, core], xh.at[layer + 1, core], x_sem.at[0, 0], x_sem.at[0, 1], partner)
    send(fin_st.at[other], fin_rc, x_sem.at[1, 0], x_sem.at[1, 1], partner)
    stores = [pltpu.make_async_copy(fin_st.at[core], hid_out.at[core], io_sem.at[0]),
              pltpu.make_async_copy(hq.at[:, :, group:group + 2], kvn_out, io_sem.at[1])]
    for copy in stores:
        copy.start()
    arrived(fin_rc, x_sem.at[1, 1], x_sem.at[1, 0])
    stores.append(pltpu.make_async_copy(fin_rc, hid_out.at[other], io_sem.at[2]))
    stores[2].start()
    for copy in stores:
        copy.wait()
    for copy in pending:
        copy.wait_send()


def cache_kernel(lens_hbm, hid, kvn, ksuf, vsuf, hid_out, kout, vout, lens, buf, tiles, hbuf, kvbuf, in_sem, out_sem, io_sem):
    layers, batch = ksuf.shape[0], ksuf.shape[1]
    heads = ksuf.shape[3]
    half = hid.shape[2]
    step = 8
    parts = batch // step
    srcs, dsts = (ksuf, vsuf), (kout, vout)

    def copies(layer, i, part, out):
        here = pl.ds(part * step, step)
        at = (layer * 2 + i) * parts + part
        if out:
            return pltpu.make_async_copy(buf.at[layer, i, here], dsts[i].at[layer, here], out_sem.at[at])
        return pltpu.make_async_copy(srcs[i].at[layer, here], buf.at[layer, i, here], in_sem.at[at])

    todo = [(layer, i, part) for layer in range(layers) for i in range(2) for part in range(parts)]
    news = pltpu.make_async_copy(kvn, kvbuf, io_sem.at[0])
    news.start()
    lengths = pltpu.make_async_copy(lens_hbm, lens, io_sem.at[4])
    lengths.start()
    ahead = len(todo) // 2
    for layer, i, part in todo[:ahead]:
        copies(layer, i, part, False).start()
    sides = [pltpu.make_async_copy(hid.at[sd], hbuf.at[:, sd * half:(sd + 1) * half], io_sem.at[1 + sd]) for sd in range(2)]
    for copy in sides:
        copy.start()
    news.wait()
    lengths.wait()
    for layer in range(layers):
        for i in range(2):
            for g in range(heads):
                tiles[layer, i, pl.ds(g, batch, stride=heads), :] = kvbuf[layer, g, i].astype(F32)
    for n, (layer, i, part) in enumerate(todo):
        copies(layer, i, part, False).wait()
        for ahead_of in todo[n + ahead:n + ahead + 1]:
            copies(*ahead_of, False).start()
        for b in range(part * step, (part + 1) * step):
            buf[layer, i, b, lens[b]] = tiles[layer, i, b * heads:(b + 1) * heads, :].astype(BF16)
        copies(layer, i, part, True).start()
    for copy in sides:
        copy.wait()
    whole = pltpu.make_async_copy(hbuf, hid_out, io_sem.at[3])
    whole.start()
    for layer, i, part in todo:
        copies(layer, i, part, True).wait()
    whole.wait()


def solution(mesh):
    ctx_size = mesh.shape["ctx"]
    home = ("data", "ctx")
    row_spec, lens_spec, whole = P(home, None), P(home), P()
    prefix_spec = P(None, home, None, None)
    cache_spec = P(None, home, None, None, None)

    def local_step(hidden, seq_lens, w_query, w_key, w_value, w_out, k_prefix, v_prefix, k_suffix, v_suffix):
        layers, dim, q_width = w_query.shape
        rows = hidden.shape[0]
        span, heads, hd = k_prefix.shape[1:]
        slots = k_suffix.shape[2]
        group = q_width // (heads * hd)
        chips = ctx_size // 2
        half, kc = dim // 2, dim // 4
        nblk = half // COLS
        qh = heads * group
        vmem, smem, anym = pltpu.VMEM, pltpu.SMEM, pl.ANY
        dma = pltpu.SemaphoreType.DMA
        spec = pl.BlockSpec
        scratch = [
            smem((rows,), jnp.int32), dma((3,)),
            vmem((RING, kc, (group + 2) * hd), BF16), dma((RING, 3)),
            vmem((chips, nblk, 2 * group * hd, COLS), BF16), dma((chips, nblk)),
            vmem((2, span, heads, hd), BF16), dma((2,)), vmem((64 * heads, hd), F32),
            vmem((layers, ctx_size, 2, span, hd), BF16), vmem((layers, 2, ctx_size, span, hd), BF16),
            dma((layers, 2, ctx_size)), dma((layers, 2, ctx_size)),
            vmem((2, rows, slots * heads, hd), BF16), dma((2,)),
            vmem((layers, 2, 2 * rows, half), BF16), vmem((2, rows, half), BF16), vmem((rows, half), BF16), dma((3, 2)),
            vmem((chips, 2 * rows, (group + 2) * hd), F32),
            vmem((layers, chips, 2, group + 2, rows, hd), BF16), vmem((layers, heads, group + 2, rows, hd), BF16),
            dma((layers, chips)), dma((layers, chips)),
            vmem((layers, chips, 2, group, rows, hd), BF16), dma((layers, chips)), dma((layers, chips)),
            vmem((rows * (qh + PAD), hd), F32), vmem((rows * (qh + PAD), hd), F32), vmem((rows * (qh + PAD), hd), F32),
            vmem((rows * qh, hd), F32),
            vmem((ctx_size, 2 * group * rows, span), F32), vmem((2 * group * rows, ctx_size * span), BF16),
            vmem((layers, chips, 2, group, rows, hd), BF16), vmem((layers, chips, 2, 8, 128), F32),
            vmem((layers, heads, group, rows, hd), BF16), vmem((layers, heads, 8, 128), F32),
            dma((layers, chips, 2)), dma((layers, heads)), dma((layers, chips, 2)), dma((layers, heads)),
            vmem((layers, 2, chips, rows, 2 * group * hd), BF16), dma((layers, chips)), dma((layers, chips)),
            vmem((nblk, 2 * rows, COLS), F32),
        ]
        hid, kvn = pl.pallas_call(
            functools.partial(decode_kernel, ctx_size),
            name="decode",
            out_shape=(jax.ShapeDtypeStruct((2, rows, half), BF16),
                       jax.ShapeDtypeStruct((layers, heads, 2, rows, hd), BF16)),
            in_specs=[spec(memory_space=anym)] * 10,
            out_specs=(spec(memory_space=anym), spec(memory_space=anym)),
            scratch_shapes=scratch,
            compiler_params=pltpu.CompilerParams(collective_id=0, has_side_effects=True, vmem_limit_bytes=67043328),
        )(hidden, seq_lens, w_query, w_key, w_value, w_out, k_prefix, v_prefix,
          k_suffix.reshape(layers, rows, slots * heads, hd), v_suffix.reshape(layers, rows, slots * heads, hd))
        copies = layers * 2 * (rows // 8)
        return pl.pallas_call(
            cache_kernel,
            name="caches",
            out_shape=(jax.ShapeDtypeStruct(hidden.shape, BF16), jax.ShapeDtypeStruct(k_suffix.shape, BF16),
                       jax.ShapeDtypeStruct(v_suffix.shape, BF16)),
            in_specs=[spec(memory_space=anym)] * 5,
            out_specs=(spec(memory_space=anym), spec(memory_space=anym), spec(memory_space=anym)),
            scratch_shapes=[smem((rows,), jnp.int32), vmem((layers, 2, rows, slots, heads, hd), BF16),
                            vmem((layers, 2, rows * heads, hd), F32),
                            vmem((rows, dim), BF16), vmem((layers, heads, 2, rows, hd), BF16),
                            dma((copies,)), dma((copies,)), dma((5,))],
            compiler_params=pltpu.CompilerParams(vmem_limit_bytes=67043328),
        )(seq_lens, hid, kvn, k_suffix, v_suffix)

    return jax.shard_map(local_step, mesh=mesh,
                         in_specs=(row_spec, lens_spec, whole, whole, whole, whole, prefix_spec, prefix_spec, cache_spec, cache_spec),
                         out_specs=(row_spec, cache_spec, cache_spec), check_vma=False)
```
